32 devices in a mesh: samp: 16 (over z, y, core), feat: 2 (over x).
Axes of the slice: x: 2, y: 2, z: 4, core: 2. Of those that a mesh axis runs over, the one named last changes fastest.
Arguments:
- grads: bfloat16 [8192, 4096], P('samp', 'feat'), may hold values from -60 to 60
- weights: float32 [8192], P('samp'), may hold values from 0.05 to 6
- targets: float32 [4096, 64], P('feat'), may hold values from -6 to 6
Outputs:
- scores: float32 [8192, 64], P(('samp', 'feat'))
- solution: float32 [4096, 64], P('feat')
- residual: float32 [4096, 64], P('feat')
The draws below stay inside these ranges and needn't reach their ends.
All inputs are finite; a program needn't handle non-finite values.
Results may differ from the reference program's by a relative error of at most 0.014.
Values may be sent and summed in bfloat16 or wider, within the bound.
A program may use at most 64 MiB of HBM per device.

```python
import math
import jax
import jax.numpy as jnp
from jax import lax

FEATURES = 4096
DIRS = 64
ITERS = 2
SAMPLES = 8192


def draw_grads(key, part):
    first = jax.random.fold_in(key, 11)
    second = jax.random.fold_in(key, 12)
    ramp = 1.0 + 2.0 * jnp.arange(FEATURES, dtype=jnp.float32) / FEATURES
    column_scale = jnp.exp(jax.random.uniform(second, (FEATURES,), jnp.float32, math.log(0.1), math.log(3.0))) * ramp
    base = jax.random.normal(first, (SAMPLES, FEATURES), jnp.float32)
    return (base * column_scale[None, :]).astype(jnp.bfloat16)


def draw_weights(key, part):
    first = jax.random.fold_in(key, 21)
    ramp = 1.0 + 2.0 * jnp.arange(SAMPLES, dtype=jnp.float32) / SAMPLES
    base = jnp.exp(jax.random.uniform(first, (SAMPLES,), jnp.float32, math.log(0.05), math.log(2.0)))
    return base * ramp


def block_scale(own_key, dims, shards, low, high):
    def one(position, parts):
        heights = jax.random.uniform(jax.random.fold_in(jax.random.fold_in(own_key, 6), position), (parts,), jnp.float32, low / len(shards), high / len(shards))
        return jnp.repeat(jnp.exp(heights), dims[position] // parts).reshape((-1,) + (1,) * (len(dims) - position - 1))

    factor_of = one(*shards[0])
    for cut in shards[1:]:
        factor_of = factor_of * one(*cut)
    return factor_of


def normal_values(stream_key, dims, deviation, limit, cuts=(), kind=jnp.bfloat16):
    loudness = block_scale(stream_key, dims, cuts, -0.22, 0.18) if cuts else 1.0
    entries = jax.random.normal(stream_key, dims, jnp.float32) * deviation * loudness
    return jnp.minimum(jnp.maximum(entries, -limit), limit).astype(kind)


def setup_inputs(seed: int = 0) -> dict:
    keys = jax.random.split(jax.random.key(seed), 4)
    return {
        "grads": draw_grads(jax.random.fold_in(keys[3], 71), 0),
        "weights": draw_weights(jax.random.fold_in(keys[3], 71), 0),
        "targets": normal_values(keys[2], (FEATURES, DIRS), 1.0, 6.0, ((0, 2),), jnp.float32),
    }


damping_term = 0.1

def apply_operator(grads, weights, vector):
    packed = vector.astype(jnp.bfloat16)
    sample_rows = jnp.dot(grads, packed, preferred_element_type=jnp.float32)
    weighted = (sample_rows * (weights / SAMPLES)[:, None]).astype(jnp.bfloat16)
    image = lax.dot_general(grads, weighted, (((0,), (0,)), ((), ())), preferred_element_type=jnp.float32)
    return (sample_rows, image + damping_term * vector)

def reference(grads, weights, targets):
    solution = jnp.zeros_like(targets)
    resid = targets
    direction = targets
    accum = jnp.zeros((grads.shape[0], targets.shape[1]), jnp.float32)
    norm_now = lax.optimization_barrier(jnp.sum(resid * resid, axis=0))
    for step in range(ITERS):
        sample_rows, image = apply_operator(grads, weights, direction)
        alpha = norm_now / lax.optimization_barrier(jnp.sum(direction * image, axis=0))
        solution = solution + alpha * direction
        resid = resid - alpha * image
        accum = accum + alpha * sample_rows
        if step + 1 < ITERS:
            norm_next = lax.optimization_barrier(jnp.sum(resid * resid, axis=0))
            direction = resid + norm_next / norm_now * direction
            norm_now = norm_next
    scores = accum / math.sqrt(FEATURES)
    return (scores, solution, resid)
```

```python
import functools
import math

import jax
import jax.numpy as jnp
from jax import lax
from jax.experimental import pallas as pl
from jax.experimental.pallas import tpu as pltpu
from jax.sharding import PartitionSpec as P

ITERS = 2
LANES = 128
VMEM_BYTES = 105 * 2**19
STORE_BYTES = 2**22
MESH = pl.DeviceIdType.MESH

damping_term = 0.1


def pack_columns(columns):
    dirs = columns[0].shape[0]
    lane = lax.broadcasted_iota(jnp.int32, (dirs, LANES), 1)
    tile = jnp.zeros((dirs, LANES), jnp.float32)
    for position, column in enumerate(columns):
        tile = jnp.where(lane == position, column, tile)
    if dirs < LANES:
        tile = jnp.concatenate([tile, jnp.zeros((LANES - dirs, LANES), jnp.float32)], axis=0)
    return tile.T[:8]


def unpack_columns(tile, count, dirs):
    padded = jnp.concatenate([tile, jnp.zeros((LANES - 8, LANES), jnp.float32)], axis=0).T
    return [padded[:dirs, i : i + 1] for i in range(count)]


def kernel(
    chips, total, full_width,
    grads_hbm, weights_hbm, targets_hbm,
    scores_ref, solution_ref, resid_ref,
    grads_ref, weights_ref, targets_ref,
    rows_out, rows_in, tile_out, tile_in,
    image_f32, image_b16, pair_in, pair_tile_out, pair_tile_in,
    chip_out, chip_in, chip_tiles, gathered,
    load_sem, feat_send, feat_recv, pair_send, pair_recv, chip_send, chip_recv,
):
    samp, feat = lax.axis_index("samp"), lax.axis_index("feat")
    core = lax.rem(samp, 2)
    chip = lax.div(samp, 2)
    dirs, width = targets_ref.shape
    rows_dev = grads_ref.shape[0]
    half = rows_dev // 2
    partner = (samp + 1 - 2 * core, feat)
    mirror = (samp, 1 - feat)
    wide_half = chips * LANES

    def peer(offset):
        other = lax.rem(chip + offset, chips)
        return other, (other * 2 + core, feat)

    loads = [
        pltpu.make_async_copy(targets_hbm, targets_ref, load_sem.at[0]),
        pltpu.make_async_copy(grads_hbm.at[pl.ds(0, half)], grads_ref.at[pl.ds(0, half)], load_sem.at[1]),
        pltpu.make_async_copy(grads_hbm.at[pl.ds(half, half)], grads_ref.at[pl.ds(half, half)], load_sem.at[2]),
        pltpu.make_async_copy(weights_hbm, weights_ref, load_sem.at[3]),
    ]
    for load in loads:
        load.start()

    barrier = pltpu.get_barrier_semaphore()
    for device in [partner, mirror] + [peer(d)[1] for d in range(1, chips)]:
        pl.semaphore_signal(barrier, inc=1, device_id=device, device_id_type=MESH)

    def remote(src, dst, send, recv, device):
        return pltpu.make_async_remote_copy(
            src_ref=src, dst_ref=dst, send_sem=send, recv_sem=recv, device_id=device, device_id_type=MESH
        )

    def lanes_of(which):
        return pl.ds(pl.multiple_of(which * wide_half, wide_half), wide_half)

    own_half, other_half = lanes_of(core), lanes_of(1 - core)
    own_lanes = pl.ds(pl.multiple_of((core * chips + chip) * LANES, LANES), LANES)
    nt = (((1,), (1,)), ((), ()))

    def joined(step, which):
        return jnp.concatenate([gathered[step, which, i] for i in range(chips)], axis=1)

    for step in range(ITERS):
        mine = []
        copies = []
        if step == 0:
            loads[0].wait()
            targets = targets_ref[...]
            packed = targets.astype(jnp.bfloat16)
        else:
            near = joined(step - 1, core)
            started = [
                lax.dot_general(
                    near, grads_ref[h * half : (h + 1) * half, own_half], nt,
                    preferred_element_type=jnp.float32)
                for h in range(2)
            ]
            for i in range(chips):
                remote(
                    gathered.at[step - 1, 1 - core, i], gathered.at[step - 1, 1 - core, i],
                    pair_send.at[step - 1, 2 + i], pair_recv.at[step - 1, 2 + i], partner).wait_recv()
            far = joined(step - 1, 1 - core)
        for h in range(2):
            rows_h = slice(h * half, (h + 1) * half)
            if step == 0:
                loads[1 + h].wait()
                part = lax.dot_general(
                    packed, grads_ref[rows_h, :], nt, preferred_element_type=jnp.float32)
            else:
                part = started[h] + lax.dot_general(
                    far, grads_ref[rows_h, other_half], nt, preferred_element_type=jnp.float32)
            rows_out[step, h] = part.astype(jnp.bfloat16)
            if step == 0 and h == 0:
                pl.semaphore_wait(barrier, chips + 1)
            copies.append(remote(
                rows_out.at[step, h], rows_in.at[step, h],
                feat_send.at[step, h], feat_recv.at[step, h], mirror))
            copies[-1].start()
            mine.append(part)
        if step == 0:
            sums = [jnp.sum(targets * targets, axis=1, keepdims=True)]
        else:
            pieces = [(near, own_half), (far, other_half)]
            sums = [0.0, 0.0]
            for block, lanes in pieces:
                block = block.astype(jnp.float32)
                sums[0] = sums[0] + jnp.sum(block * block, axis=1, keepdims=True)
                sums[1] = sums[1] + jnp.sum(block * targets_ref[:, lanes], axis=1, keepdims=True)
        tile_out[step] = pack_columns(sums)
        copies.append(remote(tile_out.at[step], tile_in.at[step], feat_send.at[step, 2], feat_recv.at[step, 2], mirror))
        copies[-1].start()
        if step == 0:
            loads[3].wait()
            scaled = weights_ref[...] / total
            target_slice = targets_ref[:, own_lanes]

        def finish_sums():
            copies[2].wait()
            return unpack_columns(tile_out[step] + tile_in[step], len(sums), dirs)

        if step == 1:
            sums = finish_sums()
            norm = sums[0]
            ratio = norm / first_norm
            square = norm + 2.0 * ratio * sums[1] + ratio * ratio * first_norm
            direction_slice = resid_slice + ratio * target_slice
        rows, curve = [], 0.0
        toward = mine_image = None
        for h in range(2):
            rows_h = slice(h * half, (h + 1) * half)
            copies[h].wait()
            whole = mine[h] + rows_in[step, h].astype(jnp.float32)
            if step == 1:
                whole = whole + ratio * first_rows[h]
            rows.append(whole)
            weighted = (whole * scaled[:, rows_h]).astype(jnp.bfloat16)
            there = jnp.dot(weighted, grads_ref[rows_h, other_half], preferred_element_type=jnp.float32)
            toward = there if h == 0 else toward + there
            if h == 1:
                for i in range(chips):
                    image_b16[step, i] = toward[:, i * LANES : (i + 1) * LANES].astype(jnp.bfloat16)
                swap = remote(image_b16.at[step], pair_in.at[step], pair_send.at[step, 0], pair_recv.at[step, 0], partner)
                swap.start()
            curve = curve + jnp.sum(weighted.astype(jnp.float32) * whole, axis=1, keepdims=True)
            if h == 1:
                pair_tile_out[step] = pack_columns([curve])
                swap_tile = remote(
                    pair_tile_out.at[step], pair_tile_in.at[step], pair_send.at[step, 1], pair_recv.at[step, 1], partner)
                swap_tile.start()
            here = jnp.dot(weighted, grads_ref[rows_h, own_half], preferred_element_type=jnp.float32)
            mine_image = here if h == 0 else mine_image + here
        if step == 0:
            first_rows = rows
            sums = finish_sums()
            first_norm = norm = square = sums[0]
            resid_slice = direction_slice = target_slice
        swap_tile.wait()
        chip_tiles[step, chip] = pair_tile_out[step] + pair_tile_in[step]
        sends = []
        for d in range(1, chips):
            other, device = peer(d)
            sends.append(remote(
                chip_tiles.at[step, chip], chip_tiles.at[step, chip],
                chip_send.at[step, 1, d], chip_recv.at[step, 1, chip], device))
            sends[-1].start()
        swap.wait()
        for i in range(chips):
            both = mine_image[:, i * LANES : (i + 1) * LANES] + pair_in[step, i].astype(jnp.float32)
            image_f32[i] = both
            chip_out[step, i] = both.astype(jnp.bfloat16)
        for d in range(1, chips):
            other, device = peer(d)
            sends.append(remote(
                chip_out.at[step, other], chip_in.at[step, chip],
                chip_send.at[step, 0, d], chip_recv.at[step, 0, chip], device))
            sends[-1].start()
        for d in range(1, chips):
            other, device = peer(d)
            remote(
                chip_tiles.at[step, other], chip_tiles.at[step, other],
                chip_send.at[step, 1, d], chip_recv.at[step, 1, other], device).wait_recv()
        curve_tile = chip_tiles[step, 0]
        for i in range(1, chips):
            curve_tile = curve_tile + chip_tiles[step, i]
        curvature = unpack_columns(curve_tile, 1, dirs)[0] + damping_term * square
        alpha = norm / curvature
        reduced = image_f32[chip] + damping_term * direction_slice
        for d in range(1, chips):
            other, device = peer(d)
            remote(
                chip_out.at[step, other], chip_in.at[step, other],
                chip_send.at[step, 0, d], chip_recv.at[step, 0, other], device).wait_recv()
            reduced = reduced + chip_in[step, other].astype(jnp.float32)
        resid_slice = resid_slice - alpha * reduced
        gathered[step, core, chip] = resid_slice.astype(jnp.bfloat16)
        spread = []
        for d in range(1, chips):
            other, device = peer(d)
            spread.append(remote(
                gathered.at[step, core, chip], gathered.at[step, core, chip],
                chip_send.at[step, 2, d], chip_recv.at[step, 2, chip], device))
            spread[-1].start()

        def forward(which):
            spread.append(remote(
                gathered.at[step, core, which], gathered.at[step, core, which],
                pair_send.at[step, 2 + which], pair_recv.at[step, 2 + which], partner))
            spread[-1].start()

        forward(chip)
        if step == 0:
            first_alpha = alpha
        else:
            scores = [
                (first_alpha * first_rows[h] + alpha * rows[h]) / math.sqrt(full_width) for h in range(2)
            ]
            scores_ref[...] = jnp.where(feat == 0, scores[0], scores[1])
            for block, lanes in pieces:
                start = targets_ref[:, lanes]
                solution_ref[:, lanes] = first_alpha * start + alpha * (block.astype(jnp.float32) + ratio * start)
        for copy in sends:
            copy.wait_send()
        for d in range(1, chips):
            other, device = peer(d)
            remote(
                gathered.at[step, core, other], gathered.at[step, core, other],
                chip_send.at[step, 2, d], chip_recv.at[step, 2, other], device).wait_recv()
            forward(other)
        if step == ITERS - 1:
            resid_ref[:, own_half] = joined(step, core).astype(jnp.float32)
            for i in range(chips):
                remote(
                    gathered.at[step, 1 - core, i], gathered.at[step, 1 - core, i],
                    pair_send.at[step, 2 + i], pair_recv.at[step, 2 + i], partner).wait_recv()
            resid_ref[:, other_half] = joined(step, 1 - core).astype(jnp.float32)
        for copy in spread:
            copy.wait_send()


def store_kernel(*refs):
    count = len(refs) // 2
    sem = refs[-1]
    copies = [pltpu.make_async_copy(refs[i], refs[count + i], sem.at[i]) for i in range(count)]
    for copy in copies:
        copy.start()
    for copy in copies:
        copy.wait()


def write_out(*arrays):
    return pl.pallas_call(
        store_kernel,
        out_shape=tuple(jax.ShapeDtypeStruct(a.shape, a.dtype) for a in arrays),
        in_specs=[pl.BlockSpec(memory_space=pltpu.VMEM)] * len(arrays),
        out_specs=[pl.BlockSpec(memory_space=pltpu.HBM)] * len(arrays),
        scratch_shapes=[pltpu.SemaphoreType.DMA((len(arrays),))],
        compiler_params=pltpu.CompilerParams(vmem_limit_bytes=STORE_BYTES),
        name="store",
    )(*arrays)


def fused(grads, weights, targets):
    rows_dev, feat_cols = grads.shape
    n_samp = lax.axis_size("samp")
    n_feat = lax.axis_size("feat")
    dirs = targets.shape[1]
    chips = n_samp // 2
    f32, b16 = jnp.float32, jnp.bfloat16
    vmem = pl.BlockSpec(memory_space=pltpu.VMEM)
    dma = pltpu.SemaphoreType.DMA
    scores, solved, resid = pl.pallas_call(
        functools.partial(kernel, chips, rows_dev * n_samp, feat_cols * n_feat),
        out_shape=(
            jax.ShapeDtypeStruct((dirs, rows_dev // n_feat), f32),
            jax.ShapeDtypeStruct((dirs, feat_cols), f32),
            jax.ShapeDtypeStruct((dirs, feat_cols), f32),
        ),
        in_specs=[pl.BlockSpec(memory_space=pltpu.HBM)] * 3,
        out_specs=[vmem] * 3,
        scratch_shapes=[
            pltpu.VMEM((rows_dev, feat_cols), b16),
            pltpu.VMEM((1, rows_dev), f32),
            pltpu.VMEM((dirs, feat_cols), f32),
            pltpu.VMEM((ITERS, 2, dirs, rows_dev // 2), b16),
            pltpu.VMEM((ITERS, 2, dirs, rows_dev // 2), b16),
            pltpu.VMEM((ITERS, 8, LANES), f32),
            pltpu.VMEM((ITERS, 8, LANES), f32),
            pltpu.VMEM((chips, dirs, LANES), f32),
            pltpu.VMEM((ITERS, chips, dirs, LANES), b16),
            pltpu.VMEM((ITERS, chips, dirs, LANES), b16),
            pltpu.VMEM((ITERS, 8, LANES), f32),
            pltpu.VMEM((ITERS, 8, LANES), f32),
            pltpu.VMEM((ITERS, chips, dirs, LANES), b16),
            pltpu.VMEM((ITERS, chips, dirs, LANES), b16),
            pltpu.VMEM((ITERS, chips, 8, LANES), f32),
            pltpu.VMEM((ITERS, 2, chips, dirs, LANES), b16),
            dma((4,)),
            dma((ITERS, 3)), dma((ITERS, 3)),
            dma((ITERS, 2 + chips)), dma((ITERS, 2 + chips)),
            dma((ITERS, 3, chips)), dma((ITERS, 3, chips)),
        ],
        compiler_params=pltpu.CompilerParams(collective_id=0, has_side_effects=True, vmem_limit_bytes=VMEM_BYTES),
        name="cg",
    )(grads, weights[None, :], targets.T)
    scores, solved, resid = write_out(scores, solved, resid)
    return scores.T, solved.T, resid.T


def per_device(grads, weights, targets):
    rows_dev, feat_cols = grads.shape
    n_samp = lax.axis_size("samp")
    n_feat = lax.axis_size("feat")
    total = rows_dev * n_samp
    full_width = feat_cols * n_feat
    share = rows_dev // n_feat
    offset = lax.axis_index("feat") * share
    scaled = weights / total
    regrouped = lax.all_to_all(grads, "feat", split_axis=0, concat_axis=1, tiled=True)
    own_weights = lax.dynamic_slice_in_dim(scaled, offset, share, 0)

    def column_norms(resid):
        squares = jnp.sum(resid * resid, axis=0)
        parts = (squares,)
        return lax.psum((parts[0],), "feat")

    solution = jnp.zeros_like(targets)
    resid = targets
    direction = targets
    accum = jnp.zeros((share, targets.shape[1]), jnp.float32)
    norm_now = column_norms(resid)[0]
    for step in range(ITERS):
        packed = direction.astype(jnp.bfloat16)
        sample_rows = jnp.dot(
            regrouped,
            lax.all_gather(packed, "feat", axis=0, tiled=True),
            preferred_element_type=jnp.float32,
        )
        weighted = (sample_rows * own_weights[:, None]).astype(jnp.bfloat16)
        partial_image = lax.psum_scatter(
            lax.dot_general(
                regrouped, weighted, (((0,), (0,)), ((), ())), preferred_element_type=jnp.float32
            ).astype(jnp.bfloat16),
            "feat",
            scatter_dimension=0,
            tiled=True,
        ).astype(jnp.float32)
        own_rows = sample_rows
        apply_own_weights = own_weights
        image = lax.psum(partial_image, "samp") + damping_term * direction
        own_rows, own_weights, image = (own_rows, apply_own_weights, image)
        curvature = lax.psum(jnp.sum(direction * image, axis=0), "feat")
        alpha = norm_now / curvature
        solution = solution + alpha * direction
        resid = resid - alpha * image
        accum = accum + alpha * own_rows
        if step + 1 < ITERS:
            sums = column_norms(resid)
            norm_next = sums[0]
            ratio = norm_next / norm_now
            direction = resid + ratio * direction
            norm_now = norm_next
    scores = accum / math.sqrt(full_width)
    return (scores, solution, resid)


def dispatch(grads, weights, targets):
    rows_dev, feat_cols = grads.shape
    n_samp, n_feat = lax.axis_size("samp"), lax.axis_size("feat")
    fits = (
        n_feat == 2
        and n_samp % 2 == 0
        and n_samp >= 4
        and feat_cols == n_samp * LANES
        and rows_dev % (2 * LANES) == 0
        and targets.shape[1] % 16 == 0
        and targets.shape[1] <= LANES
    )
    return (fused if fits else per_device)(grads, weights, targets)


def solution(mesh):
    return jax.shard_map(
        dispatch,
        mesh=mesh,
        in_specs=(P("samp", "feat"), P("samp"), P("feat", None)),
        out_specs=(P(("samp", "feat"), None), P("feat", None), P("feat", None)),
        check_vma=False,
    )
```

```python
import functools
import math

import jax
import jax.numpy as jnp
from jax import lax
from jax.experimental import pallas as pl
from jax.experimental.pallas import tpu as pltpu
from jax.sharding import PartitionSpec as P

ITERS = 2
CHUNK = 16
LANES = 128
VMEM_BYTES = 105 * 2**19
STORE_BYTES = 2**22
MESH = pl.DeviceIdType.MESH

damping_term = 0.1


def kernel(
    total, full_width,
    grads_hbm, weights_hbm, targets_hbm,
    scores_ref, solution_ref, resid_ref,
    grads_ref, weights_ref, targets_ref,
    rows_out, rows_in, first_rows, second_rows,
    norms_out, norms_in, sums_out, sums_in,
    part_out, part_in, gathered, curve_out, curve_in,
    load_sem, x_send, x_recv, part_send, part_recv, gather_send, gather_recv, curve_send, curve_recv,
):
    samp, feat = lax.axis_index("samp"), lax.axis_index("feat")
    n_samp = part_in.shape[1]
    chips = n_samp // 2
    core, chip = lax.rem(samp, 2), lax.div(samp, 2)
    dirs = targets_ref.shape[0]
    rows_dev = grads_ref.shape[0]
    half = rows_dev // 2
    pair = 2 * LANES
    groups = [slice(i, min(i + CHUNK, dirs)) for i in range(0, dirs, CHUNK)]
    count = len(groups)
    f32, b16 = jnp.float32, jnp.bfloat16
    nt = (((1,), (1,)), ((), ()))
    mirror = (samp, 1 - feat)

    def flipped(index, mask, bits):
        for b in range(bits):
            if (mask >> b) & 1:
                index = index + (1 - 2 * lax.rem(lax.div(index, 2**b), 2)) * 2**b
        return index

    bits = (chips - 1).bit_length()
    peer_chip = [flipped(chip, j, bits) for j in range(chips)]
    near_first = sorted(range(chips), key=lambda j: j // 2 + j % 2)
    far_first = near_first[::-1]

    def peer(j, c):
        to = core if c == 0 else 1 - core
        return to, (peer_chip[j] * 2 + to, feat)

    others = [(j, c) for j in far_first for c in (0, 1) if (j, c) != (0, 0)]

    loads = [
        pltpu.make_async_copy(targets_hbm, targets_ref, load_sem.at[0]),
        pltpu.make_async_copy(grads_hbm.at[pl.ds(0, half)], grads_ref.at[pl.ds(0, half)], load_sem.at[1]),
        pltpu.make_async_copy(grads_hbm.at[pl.ds(half, half)], grads_ref.at[pl.ds(half, half)], load_sem.at[2]),
        pltpu.make_async_copy(weights_hbm, weights_ref, load_sem.at[3]),
    ]
    for load in loads:
        load.start()

    barrier = pltpu.get_barrier_semaphore()
    for device in [mirror] + [peer(j, c)[1] for j, c in others]:
        pl.semaphore_signal(barrier, inc=1, device_id=device, device_id_type=MESH)

    def remote(src, dst, send, recv, device):
        return pltpu.make_async_remote_copy(
            src_ref=src, dst_ref=dst, send_sem=send, recv_sem=recv, device_id=device, device_id_type=MESH
        )

    def rows_of(g):
        return pl.ds(groups[g].start, groups[g].stop - groups[g].start)

    def pair_lanes(j):
        return pl.ds(pl.multiple_of(peer_chip[j] * pair, pair), pair)

    own_lanes = pl.ds(pl.multiple_of(samp * LANES, LANES), LANES)

    def x_copy(s, g, kind):
        if kind == 0:
            src, dst = rows_out.at[s, rows_of(g)], rows_in.at[s, rows_of(g)]
        elif s == 0:
            src, dst = norms_out.at[rows_of(g)], norms_in.at[rows_of(g)]
        else:
            src, dst = sums_out.at[rows_of(g)], sums_in.at[rows_of(g)]
        return remote(src, dst, x_send.at[s, g, kind], x_recv.at[s, g, kind], mirror)

    def part_copy(s, g, j, c):
        to, device = peer(j, c)
        return remote(
            part_out.at[s, j, to, rows_of(g)], part_in.at[s, 2 * j + c, rows_of(g)],
            part_send.at[s, g], part_recv.at[s, g], device)

    def part_all(s, g):
        ref = part_in.at[s, pl.ds(1, n_samp - 1), rows_of(g)]
        return remote(ref, ref, part_send.at[s, g], part_recv.at[s, g], mirror)

    def tile_copy(s, g, j, c):
        to, device = peer(j, c)
        ref = gathered.at[s, chip, core, rows_of(g)]
        return remote(ref, ref, gather_send.at[s, g], gather_recv.at[s, g, j], device)

    def tile_wait(s, g, j):
        if j == 0:
            ref = gathered.at[s, chip, 1 - core, rows_of(g)]
        else:
            ref = gathered.at[s, peer_chip[j], pl.ds(0, 2), rows_of(g)]
        remote(ref, ref, gather_send.at[s, g], gather_recv.at[s, g, j], mirror).wait_recv()

    def curve_copy(g, j, c):
        to, device = peer(j, c)
        return remote(
            curve_out.at[g, pl.ds(0, 1)], curve_in.at[g, pl.ds(2 * j + c, 1)],
            curve_send.at[g], curve_recv.at[g], device)

    def curve_all(g):
        ref = curve_in.at[g, pl.ds(1, n_samp - 1)]
        return remote(ref, ref, curve_send.at[g], curve_recv.at[g], mirror)

    def lane_sum(block):
        folded = block[:, :LANES]
        for i in range(1, block.shape[1] // LANES):
            folded = folded + block[:, i * LANES : (i + 1) * LANES]
        return folded

    def column(block):
        return jnp.sum(block, axis=1, keepdims=True)

    def diagonal(size):
        shape = (size, LANES)
        return lax.broadcasted_iota(jnp.int32, shape, 0) == lax.broadcasted_iota(jnp.int32, shape, 1)

    loads[0].wait()
    targets = targets_ref[...]
    packed = targets.astype(b16)
    for h in range(2):
        part_h = slice(h * half, (h + 1) * half)
        loads[1 + h].wait()
        part = lax.dot_general(packed, grads_ref[part_h, :], nt, preferred_element_type=f32)
        first_rows[:, part_h] = part
        rows_out[0, :, part_h] = part.astype(b16)
    pl.semaphore_wait(barrier, n_samp)
    for g in range(count):
        x_copy(0, g, 0).start()
    norms_out[...] = lane_sum(targets * targets)
    for g in range(count):
        x_copy(0, g, 1).start()
    loads[3].wait()
    scaled = weights_ref[...] / total
    state = [dict() for _ in range(count)]

    def exchange(s, g):
        now, rows = state[g], groups[g]
        if s == 0:
            x_copy(0, g, 0).wait_recv()
            whole = first_rows[rows, :] + rows_in[0, rows, :].astype(f32)
            first_rows[rows, :] = whole
        else:
            x_copy(0, g, 1).wait_recv()
            x_copy(1, g, 1).wait_recv()
            norm0 = column(norms_out[rows, :] + norms_in[rows, :])
            both = sums_out[rows, :] + sums_in[rows, :]
            along, square = column(both[:, :LANES]), column(both[:, LANES:])
            alpha0 = norm0 / along
            cross = norm0 - alpha0 * along
            norm1 = cross - alpha0 * (along - alpha0 * square)
            ratio = norm1 / norm0
            now.update(alpha0=alpha0, norm1=norm1, ratio=ratio,
                       length=norm1 + 2.0 * ratio * cross + ratio * ratio * norm0)
            x_copy(1, g, 0).wait_recv()
            image_rows = second_rows[rows, :] + rows_in[1, rows, :].astype(f32)
            whole = (1.0 + ratio) * first_rows[rows, :] - alpha0 * image_rows
            second_rows[rows, :] = whole
        weighted = (whole * scaled).astype(b16)
        for j in far_first:
            image = jnp.dot(weighted, grads_ref[:, pair_lanes(j)], preferred_element_type=f32)
            if j == 0:
                now["own"] = jnp.where(core == 0, image[:, :LANES], image[:, LANES:])
            for c in range(2):
                part_out[s, j, c, rows, :] = image[:, c * LANES : (c + 1) * LANES].astype(b16)
            for c in range(2):
                if (j, c) != (0, 0):
                    part_copy(s, g, j, c).start()
        if s == 1:
            size = rows.stop - rows.start
            curve = column(lane_sum(weighted.astype(f32) * whole))
            line = jnp.sum(jnp.where(diagonal(size), curve, 0.0), axis=0, keepdims=True)
            curve_out[g, 0:1, :] = line
            curve_in[g, 0:1, :] = line
            for j, c in others:
                curve_copy(g, j, c).start()

    def reduce(s, g):
        now, rows = state[g], groups[g]
        target = targets_ref[rows, own_lanes]
        if s == 1:
            curve_all(g).wait_recv()
            size = rows.stop - rows.start
            line = jnp.sum(curve_in[g], axis=0, keepdims=True)
            curve = column(jnp.where(diagonal(size), line, 0.0))
            now["alpha1"] = now["norm1"] / (curve + damping_term * now["length"])
            resid = target - now["alpha0"] * now["image0"]
            direction = resid + now["ratio"] * target
        else:
            direction = target
        part_all(s, g).wait_recv()
        image = now["own"] + damping_term * direction
        for k in range(1, n_samp):
            image = image + part_in[s, k, rows, :].astype(f32)
        if s == 0:
            now["image0"] = image
            tile = image
        else:
            tile = resid - now["alpha1"] * image
        gathered[s, chip, core, rows, :] = tile.astype(b16)
        for j, c in others:
            tile_copy(s, g, j, c).start()

    def gather(s, g):
        now, rows = state[g], groups[g]
        if s == 0:
            mine = along = square = 0.0
            for j in near_first:
                tile_wait(0, g, j)
                block = jnp.concatenate([gathered[0, peer_chip[j], c, rows, :] for c in range(2)], axis=1)
                mine = mine + lax.dot_general(
                    block, grads_ref[:, pair_lanes(j)], nt, preferred_element_type=f32)
                block = block.astype(f32)
                along = along + lane_sum(block * targets_ref[rows, pair_lanes(j)])
                square = square + lane_sum(block * block)
            sums_out[rows, :] = jnp.concatenate([along, square], axis=1)
            x_copy(1, g, 1).start()
            rows_out[1, rows, :] = mine.astype(b16)
            x_copy(1, g, 0).start()
            second_rows[rows, :] = mine
        else:
            for j in near_first:
                tile_wait(1, g, j)
                for c in range(2):
                    lanes = pl.ds(pl.multiple_of(peer_chip[j] * pair + c * LANES, LANES), LANES)
                    resid_ref[rows, lanes] = gathered[1, peer_chip[j], c, rows, :].astype(f32)

    def finish(g):
        now, rows = state[g], groups[g]
        alpha0, alpha1 = now["alpha0"], now["alpha1"]
        share = rows_dev // 2
        scores = (alpha0 * first_rows[rows, :] + alpha1 * second_rows[rows, :]) / math.sqrt(full_width)
        scores_ref[rows, :] = jnp.where(feat == 0, scores[:, :share], scores[:, share:])
        start_part = alpha0 + alpha1 * (1.0 + now["ratio"])
        image_part = alpha1 * alpha0
        for i in range(chips):
            for c in range(2):
                lanes = slice(i * pair + c * LANES, i * pair + (c + 1) * LANES)
                solution_ref[rows, lanes] = (
                    start_part * targets_ref[rows, lanes] - image_part * gathered[0, i, c, rows, :].astype(f32))

    for step in order(count):
        stage, *where = step
        {"exchange": exchange, "reduce": reduce, "gather": gather, "finish": finish}[stage](*where)
    for g in range(count):
        for s in range(ITERS):
            for kind in range(2):
                x_copy(s, g, kind).wait_send()
            part_all(s, g).wait_send()
            part_ref = part_in.at[s, pl.ds(1, n_samp - 1), rows_of(g)]
            remote(part_ref, part_ref, gather_send.at[s, g], gather_send.at[s, g], mirror).wait_send()
        curve_all(g).wait_send()


def order(count):
    steps = []
    all_of = range(count)
    steps += [("exchange", 0, g) for g in all_of]
    steps += [("reduce", 0, g) for g in all_of]
    lag = max(1, count - 1)
    gathers, exchanges = list(all_of), list(all_of)
    steps += [("gather", 0, g) for g in gathers[:lag]]
    for g in exchanges:
        steps.append(("exchange", 1, g))
        if lag + g < count:
            steps.append(("gather", 0, lag + g))
    steps += [("reduce", 1, g) for g in all_of]
    steps += [("finish", g) for g in all_of]
    steps += [("gather", 1, g) for g in all_of]
    return steps


def store_kernel(*refs):
    count = len(refs) // 2
    sem = refs[-1]
    copies = [pltpu.make_async_copy(refs[i], refs[count + i], sem.at[i]) for i in range(count)]
    for copy in copies:
        copy.start()
    for copy in copies:
        copy.wait()


def write_out(*arrays):
    return pl.pallas_call(
        store_kernel,
        out_shape=tuple(jax.ShapeDtypeStruct(a.shape, a.dtype) for a in arrays),
        in_specs=[pl.BlockSpec(memory_space=pltpu.VMEM)] * len(arrays),
        out_specs=[pl.BlockSpec(memory_space=pltpu.HBM)] * len(arrays),
        scratch_shapes=[pltpu.SemaphoreType.DMA((len(arrays),))],
        compiler_params=pltpu.CompilerParams(vmem_limit_bytes=STORE_BYTES),
        name="store",
    )(*arrays)


def fused(grads, weights, targets):
    rows_dev, feat_cols = grads.shape
    n_samp = lax.axis_size("samp")
    n_feat = lax.axis_size("feat")
    dirs = targets.shape[1]
    chips = n_samp // 2
    count = -(-dirs // CHUNK)
    f32, b16 = jnp.float32, jnp.bfloat16
    vmem = pl.BlockSpec(memory_space=pltpu.VMEM)
    dma = pltpu.SemaphoreType.DMA
    scores, solved, resid = pl.pallas_call(
        functools.partial(kernel, rows_dev * n_samp, feat_cols * n_feat),
        out_shape=(
            jax.ShapeDtypeStruct((dirs, rows_dev // n_feat), f32),
            jax.ShapeDtypeStruct((dirs, feat_cols), f32),
            jax.ShapeDtypeStruct((dirs, feat_cols), f32),
        ),
        in_specs=[pl.BlockSpec(memory_space=pltpu.HBM)] * 3,
        out_specs=[vmem] * 3,
        scratch_shapes=[
            pltpu.VMEM((rows_dev, feat_cols), b16),
            pltpu.VMEM((1, rows_dev), f32),
            pltpu.VMEM((dirs, feat_cols), f32),
            pltpu.VMEM((ITERS, dirs, rows_dev), b16),
            pltpu.VMEM((ITERS, dirs, rows_dev), b16),
            pltpu.VMEM((dirs, rows_dev), f32),
            pltpu.VMEM((dirs, rows_dev), f32),
            pltpu.VMEM((dirs, LANES), f32),
            pltpu.VMEM((dirs, LANES), f32),
            pltpu.VMEM((dirs, 2 * LANES), f32),
            pltpu.VMEM((dirs, 2 * LANES), f32),
            pltpu.VMEM((ITERS, chips, 2, dirs, LANES), b16),
            pltpu.VMEM((ITERS, n_samp, dirs, LANES), b16),
            pltpu.VMEM((ITERS, chips, 2, dirs, LANES), b16),
            pltpu.VMEM((count, 8, LANES), f32),
            pltpu.VMEM((count, n_samp, LANES), f32),
            dma((4,)),
            dma((ITERS, count, 2)), dma((ITERS, count, 2)),
            dma((ITERS, count)), dma((ITERS, count)),
            dma((ITERS, count)), dma((ITERS, count, chips)),
            dma((count,)), dma((count,)),
        ],
        compiler_params=pltpu.CompilerParams(collective_id=0, has_side_effects=True, vmem_limit_bytes=VMEM_BYTES),
        name="cg",
    )(grads, pltpu.with_memory_space_constraint(weights[None, :], pltpu.HBM), targets.T)
    scores, solved, resid = write_out(scores, solved, resid)
    return scores.T, solved.T, resid.T


def per_device(grads, weights, targets):
    rows_dev, feat_cols = grads.shape
    n_samp = lax.axis_size("samp")
    n_feat = lax.axis_size("feat")
    total = rows_dev * n_samp
    full_width = feat_cols * n_feat
    share = rows_dev // n_feat
    offset = lax.axis_index("feat") * share
    scaled = weights / total
    regrouped = lax.all_to_all(grads, "feat", split_axis=0, concat_axis=1, tiled=True)
    own_weights = lax.dynamic_slice_in_dim(scaled, offset, share, 0)

    def column_norms(resid):
        squares = jnp.sum(resid * resid, axis=0)
        parts = (squares,)
        return lax.psum((parts[0],), "feat")

    solution = jnp.zeros_like(targets)
    resid = targets
    direction = targets
    accum = jnp.zeros((share, targets.shape[1]), jnp.float32)
    norm_now = column_norms(resid)[0]
    for step in range(ITERS):
        packed = direction.astype(jnp.bfloat16)
        sample_rows = jnp.dot(
            regrouped,
            lax.all_gather(packed, "feat", axis=0, tiled=True),
            preferred_element_type=jnp.float32,
        )
        weighted = (sample_rows * own_weights[:, None]).astype(jnp.bfloat16)
        partial_image = lax.psum_scatter(
            lax.dot_general(
                regrouped, weighted, (((0,), (0,)), ((), ())), preferred_element_type=jnp.float32
            ).astype(jnp.bfloat16),
            "feat",
            scatter_dimension=0,
            tiled=True,
        ).astype(jnp.float32)
        own_rows = sample_rows
        apply_own_weights = own_weights
        image = lax.psum(partial_image, "samp") + damping_term * direction
        own_rows, own_weights, image = (own_rows, apply_own_weights, image)
        curvature = lax.psum(jnp.sum(direction * image, axis=0), "feat")
        alpha = norm_now / curvature
        solution = solution + alpha * direction
        resid = resid - alpha * image
        accum = accum + alpha * own_rows
        if step + 1 < ITERS:
            sums = column_norms(resid)
            norm_next = sums[0]
            ratio = norm_next / norm_now
            direction = resid + ratio * direction
            norm_now = norm_next
    scores = accum / math.sqrt(full_width)
    return (scores, solution, resid)


def dispatch(grads, weights, targets):
    rows_dev, feat_cols = grads.shape
    n_samp, n_feat = lax.axis_size("samp"), lax.axis_size("feat")
    fits = (
        n_feat == 2
        and n_samp >= 4
        and n_samp & (n_samp - 1) == 0
        and feat_cols == n_samp * LANES
        and rows_dev % (2 * LANES) == 0
        and targets.shape[1] % CHUNK == 0
        and targets.shape[1] <= LANES
    )
    return (fused if fits else per_device)(grads, weights, targets)


def solution(mesh):
    return jax.shard_map(
        dispatch,
        mesh=mesh,
        in_specs=(P("samp", "feat"), P("samp"), P("feat", None)),
        out_specs=(P(("samp", "feat"), None), P("feat", None), P("feat", None)),
        check_vma=False,
    )
```

```python
import functools
import math

import jax
import jax.numpy as jnp
from jax import lax
from jax.experimental import pallas as pl
from jax.experimental.pallas import tpu as pltpu
from jax.sharding import PartitionSpec as P

ITERS = 2
CHUNK = 32
GATHER_CUTS = (5,)
PART_HOPS = 4
TILE_HOPS = 4
LANES = 128
VMEM_BYTES = 105 * 2**19
STORE_BYTES = 2**22
MESH = pl.DeviceIdType.MESH

damping_term = 0.1


def kernel(
    total, full_width,
    grads_hbm, weights_hbm, targets_hbm,
    scores_ref, solution_ref, resid_ref,
    grads_ref, weights_ref, targets_ref,
    rows_out, rows_in, first_rows, second_rows,
    norms_out, norms_in, sums_out, sums_in,
    swap_out, swap_in, near_f32, near_out, part_out, part_in, gathered, curve_out, curve_in,
    load_sem, x_send, x_recv, swap_send, swap_recv, part_send, part_recv,
    gather_send, gather_recv, pass_send, pass_recv, curve_send, curve_recv,
):
    samp, feat = lax.axis_index("samp"), lax.axis_index("feat")
    n_samp = curve_in.shape[1]
    chips = n_samp // 2
    core, chip = lax.rem(samp, 2), lax.div(samp, 2)
    dirs = targets_ref.shape[0]
    rows_dev = grads_ref.shape[0]
    half = rows_dev // 2
    pair = 2 * LANES
    groups = [slice(i, min(i + CHUNK, dirs)) for i in range(0, dirs, CHUNK)]
    count = len(groups)
    f32, b16 = jnp.float32, jnp.bfloat16
    nt = (((1,), (1,)), ((), ()))
    mirror = (samp, 1 - feat)

    def flipped(index, mask, bits):
        for b in range(bits):
            if (mask >> b) & 1:
                index = index + (1 - 2 * lax.rem(lax.div(index, 2**b), 2)) * 2**b
        return index

    bits = (chips - 1).bit_length()
    peer_chip = [flipped(chip, j, bits) for j in range(chips)]
    near_first = hop_order(chips)
    far_first = near_first[::-1]
    direct, near = split_hops(chips, PART_HOPS)
    wide, narrow = split_hops(chips, TILE_HOPS)
    partner = (chip * 2 + 1 - core, feat)

    def peer(j, c):
        to = core if c == 0 else 1 - core
        return to, (peer_chip[j] * 2 + to, feat)

    others = [(j, c) for j in far_first for c in (0, 1) if (j, c) != (0, 0)]

    loads = [
        pltpu.make_async_copy(targets_hbm, targets_ref, load_sem.at[0]),
        pltpu.make_async_copy(grads_hbm.at[pl.ds(0, half)], grads_ref.at[pl.ds(0, half)], load_sem.at[1]),
        pltpu.make_async_copy(grads_hbm.at[pl.ds(half, half)], grads_ref.at[pl.ds(half, half)], load_sem.at[2]),
        pltpu.make_async_copy(weights_hbm, weights_ref, load_sem.at[3]),
    ]
    for load in loads:
        load.start()

    barrier = pltpu.get_barrier_semaphore()
    for device in [mirror] + [peer(j, c)[1] for j, c in others]:
        pl.semaphore_signal(barrier, inc=1, device_id=device, device_id_type=MESH)

    def remote(src, dst, send, recv, device):
        return pltpu.make_async_remote_copy(
            src_ref=src, dst_ref=dst, send_sem=send, recv_sem=recv, device_id=device, device_id_type=MESH
        )

    def rows_of(g):
        return pl.ds(groups[g].start, groups[g].stop - groups[g].start)

    def pair_lanes(j):
        return pl.ds(pl.multiple_of(peer_chip[j] * pair, pair), pair)

    own_lanes = pl.ds(pl.multiple_of(samp * LANES, LANES), LANES)

    def x_copy(s, g, kind):
        if kind == 0:
            src, dst = rows_out.at[s, rows_of(g)], rows_in.at[s, rows_of(g)]
        elif s == 0:
            src, dst = norms_out.at[rows_of(g)], norms_in.at[rows_of(g)]
        else:
            src, dst = sums_out.at[g, pl.ds(0, 2)], sums_in.at[g, pl.ds(0, 2)]
        return remote(src, dst, x_send.at[s, g, kind], x_recv.at[s, g, kind], mirror)

    def size_of(g):
        return groups[g].stop - groups[g].start

    def swap_copy(s, g):
        return remote(
            swap_out.at[s, 1 - core, :, rows_of(g)], swap_in.at[s, :, rows_of(g)],
            swap_send.at[s, g], swap_recv.at[s, g], partner)

    def part_copy(s, g, j, c):
        to, device = peer(j, c)
        if j in near:
            place = near.index(j) - 1
            src, slot = near_out.at[s, place, rows_of(g)], 2 * len(direct) + place
        else:
            src, slot = part_out.at[s, direct.index(j), to, rows_of(g)], 2 * direct.index(j) + c
        return remote(src, part_in.at[s, slot, rows_of(g)], part_send.at[s, g], part_recv.at[s, g], device)

    def part_all(s, g):
        ref = part_in.at[s, :, rows_of(g)]
        return remote(ref, ref, part_send.at[s, g], part_recv.at[s, g], mirror)

    def tile_copy(s, g, j, c):
        to, device = peer(j, c)
        ref = gathered.at[s, chip, core, rows_of(g)]
        return remote(ref, ref, gather_send.at[s, g], gather_recv.at[s, g, j], device)

    def tile_sends(s, g):
        sends = [(j, 0) for j in far_first if j in narrow and j] + [(0, 1)]
        return [tile_copy(s, g, j, c) for j in wide for c in (0, 1)] + [tile_copy(s, g, j, c) for j, c in sends]

    def pass_copy(s, g, j):
        ref = gathered.at[s, peer_chip[j], core, rows_of(g)]
        return remote(ref, ref, pass_send.at[s, g], pass_recv.at[s, g, j], partner)

    def tile_arrival(s, g, j):
        if j == 0:
            ref = gathered.at[s, chip, 1 - core, rows_of(g)]
        elif j in narrow:
            ref = gathered.at[s, peer_chip[j], core, rows_of(g)]
        else:
            ref = gathered.at[s, peer_chip[j], pl.ds(0, 2), rows_of(g)]
        remote(ref, ref, gather_send.at[s, g], gather_recv.at[s, g, j], mirror).wait_recv()

    def tile_wait(s, g, j):
        if j == 0 or j in wide:
            tile_arrival(s, g, j)
        else:
            ref = gathered.at[s, peer_chip[j], 1 - core, rows_of(g)]
            remote(ref, ref, pass_send.at[s, g], pass_recv.at[s, g, j], partner).wait_recv()

    def forward(s, g):
        for j in near_first:
            if j in narrow and j:
                tile_arrival(s, g, j)
                pass_copy(s, g, j).start()

    def curve_copy(g, j, c):
        to, device = peer(j, c)
        return remote(
            curve_out.at[g, pl.ds(0, 1)], curve_in.at[g, pl.ds(2 * j + c, 1)],
            curve_send.at[g], curve_recv.at[g], device)

    def curve_all(g):
        ref = curve_in.at[g, pl.ds(1, n_samp - 1)]
        return remote(ref, ref, curve_send.at[g], curve_recv.at[g], mirror)

    def lane_sum(block):
        folded = block[:, :LANES]
        for i in range(1, block.shape[1] // LANES):
            folded = folded + block[:, i * LANES : (i + 1) * LANES]
        return folded

    def column(block):
        return jnp.sum(block, axis=1, keepdims=True)

    def diagonal(size):
        shape = (size, LANES)
        return lax.broadcasted_iota(jnp.int32, shape, 0) == lax.broadcasted_iota(jnp.int32, shape, 1)

    def to_line(values, size):
        return jnp.sum(jnp.where(diagonal(size), values, 0.0), axis=0, keepdims=True)

    def to_column(line, size):
        return column(jnp.where(diagonal(size), line, 0.0))

    loads[0].wait()
    targets = targets_ref[...]
    packed = targets.astype(b16)
    for h in range(2):
        part_h = slice(h * half, (h + 1) * half)
        loads[1 + h].wait()
        part = lax.dot_general(packed, grads_ref[part_h, :], nt, preferred_element_type=f32)
        first_rows[:, part_h] = part
        rows_out[0, :, part_h] = part.astype(b16)
    pl.semaphore_wait(barrier, n_samp)
    for g in range(count):
        x_copy(0, g, 0).start()
    norms_out[...] = lane_sum(targets * targets)
    for g in range(count):
        x_copy(0, g, 1).start()
    loads[3].wait()
    scaled = weights_ref[...] / total
    state = [dict() for _ in range(count)]

    def exchange(s, g):
        now, rows = state[g], groups[g]
        if s == 0:
            x_copy(0, g, 0).wait_recv()
            whole = first_rows[rows, :] + rows_in[0, rows, :].astype(f32)
            first_rows[rows, :] = whole
        else:
            x_copy(0, g, 1).wait_recv()
            x_copy(1, g, 1).wait_recv()
            norm0 = column(norms_out[rows, :] + norms_in[rows, :])
            both = sums_out[g, 0:2, :] + sums_in[g, 0:2, :]
            along, square = [to_column(both[i : i + 1], size_of(g)) for i in range(2)]
            alpha0 = norm0 / along
            cross = norm0 - alpha0 * along
            norm1 = cross - alpha0 * (along - alpha0 * square)
            ratio = norm1 / norm0
            now.update(alpha0=alpha0, norm1=norm1, ratio=ratio,
                       length=norm1 + 2.0 * ratio * cross + ratio * ratio * norm0)
            x_copy(1, g, 0).wait_recv()
            image_rows = second_rows[rows, :] + rows_in[1, rows, :].astype(f32)
            whole = (1.0 + ratio) * first_rows[rows, :] - alpha0 * image_rows
            second_rows[rows, :] = whole
        weighted = (whole * scaled).astype(b16)
        for j in far_first:
            image = jnp.dot(weighted, grads_ref[:, pair_lanes(j)], preferred_element_type=f32)
            tiles = [image[:, c * LANES : (c + 1) * LANES] for c in range(2)]
            if j in near:
                near_f32[near.index(j), rows, :] = jnp.where(core == 0, tiles[0], tiles[1])
            for c in range(2):
                if j in near:
                    swap_out[s, c, near.index(j), rows, :] = tiles[c].astype(b16)
                else:
                    part_out[s, direct.index(j), c, rows, :] = tiles[c].astype(b16)
        swap_copy(s, g).start()
        for j in direct:
            for c in range(2):
                part_copy(s, g, j, c).start()
        if s == 1:
            line = to_line(column(lane_sum(weighted.astype(f32) * whole)), size_of(g))
            curve_out[g, 0:1, :] = line
            curve_in[g, 0:1, :] = line
            for j, c in others:
                curve_copy(g, j, c).start()

    def swap(s, g):
        now, rows = state[g], groups[g]
        swap_copy(s, g).wait_recv()
        for place, j in reversed(list(enumerate(near))):
            both = near_f32[place, rows, :] + swap_in[s, place, rows, :].astype(f32)
            if j:
                near_out[s, place - 1, rows, :] = both.astype(b16)
                part_copy(s, g, j, 0).start()
            else:
                now["own"] = both

    def reduce(s, g):
        now, rows = state[g], groups[g]
        target = targets_ref[rows, own_lanes]
        if s == 1:
            curve_all(g).wait_recv()
            curve = to_column(jnp.sum(curve_in[g], axis=0, keepdims=True), size_of(g))
            now["alpha1"] = now["norm1"] / (curve + damping_term * now["length"])
            resid = target - now["alpha0"] * now["image0"]
            direction = resid + now["ratio"] * target
        else:
            direction = target
        part_all(s, g).wait_recv()
        image = now["own"] + damping_term * direction
        for k in range(part_in.shape[1]):
            image = image + part_in[s, k, rows, :].astype(f32)
        if s == 0:
            now["image0"] = image
            tile = image
        else:
            tile = resid - now["alpha1"] * image
        gathered[s, chip, core, rows, :] = tile.astype(b16)
        for copy in tile_sends(s, g):
            copy.start()

    def gather(s, g):
        now, rows = state[g], groups[g]
        if s == 0:
            mine = along = square = 0.0
            for place, j in enumerate(near_first):
                for first, last in zip((0,) + GATHER_CUTS, GATHER_CUTS + (chips,)):
                    if place == first:
                        for other in near_first[first:last]:
                            tile_wait(0, g, other)
                block = jnp.concatenate([gathered[0, peer_chip[j], c, rows, :] for c in range(2)], axis=1)
                mine = mine + lax.dot_general(
                    block, grads_ref[:, pair_lanes(j)], nt, preferred_element_type=f32)
                block = block.astype(f32)
                along = along + lane_sum(block * targets_ref[rows, pair_lanes(j)])
                square = square + lane_sum(block * block)
            for i, block in enumerate([along, square]):
                sums_out[g, i : i + 1, :] = to_line(column(block), size_of(g))
            x_copy(1, g, 1).start()
            rows_out[1, rows, :] = mine.astype(b16)
            x_copy(1, g, 0).start()
            second_rows[rows, :] = mine
        else:
            for j in near_first:
                tile_wait(1, g, j)
                for c in range(2):
                    lanes = pl.ds(pl.multiple_of(peer_chip[j] * pair + c * LANES, LANES), LANES)
                    resid_ref[rows, lanes] = gathered[1, peer_chip[j], c, rows, :].astype(f32)

    def finish(g):
        now, rows = state[g], groups[g]
        alpha0, alpha1 = now["alpha0"], now["alpha1"]
        share = rows_dev // 2
        scores = (alpha0 * first_rows[rows, :] + alpha1 * second_rows[rows, :]) / math.sqrt(full_width)
        scores_ref[rows, :] = jnp.where(feat == 0, scores[:, :share], scores[:, share:])
        start_part = alpha0 + alpha1 * (1.0 + now["ratio"])
        image_part = alpha1 * alpha0
        for i in range(chips):
            for c in range(2):
                lanes = slice(i * pair + c * LANES, i * pair + (c + 1) * LANES)
                solution_ref[rows, lanes] = (
                    start_part * targets_ref[rows, lanes] - image_part * gathered[0, i, c, rows, :].astype(f32))

    stages = dict(exchange=exchange, swap=swap, reduce=reduce, forward=forward, gather=gather, finish=finish)
    for step in order(count):
        stage, *where = step
        stages[stage](*where)
    for g in range(count):
        for s in range(ITERS):
            for kind in range(2):
                x_copy(s, g, kind).wait_send()
            swap_copy(s, g).wait_send()
            part_all(s, g).wait_send()
            for copy in tile_sends(s, g):
                copy.wait_send()
            for j in narrow:
                if j:
                    pass_copy(s, g, j).wait_send()
        curve_all(g).wait_send()


def hop_order(chips):
    return sorted(range(chips), key=hops)


def hops(j):
    return j // 2 + j % 2


def split_hops(chips, limit):
    ordered = hop_order(chips)
    return [j for j in ordered if hops(j) >= limit], [j for j in ordered if hops(j) < limit]


def order(count):
    steps = []
    for s in range(ITERS):
        for stage in ("exchange", "swap", "reduce"):
            steps += [(stage, s, g) for g in range(count)]
        if s == ITERS - 1:
            steps += [("finish", g) for g in range(count)]
        for stage in ("forward", "gather"):
            steps += [(stage, s, g) for g in range(count)]
    return steps


def store_kernel(*refs):
    count = len(refs) // 2
    sem = refs[-1]
    copies = [pltpu.make_async_copy(refs[i], refs[count + i], sem.at[i]) for i in range(count)]
    for copy in copies:
        copy.start()
    for copy in copies:
        copy.wait()


def write_out(*arrays):
    return pl.pallas_call(
        store_kernel,
        out_shape=tuple(jax.ShapeDtypeStruct(a.shape, a.dtype) for a in arrays),
        in_specs=[pl.BlockSpec(memory_space=pltpu.VMEM)] * len(arrays),
        out_specs=[pl.BlockSpec(memory_space=pltpu.HBM)] * len(arrays),
        scratch_shapes=[pltpu.SemaphoreType.DMA((len(arrays),))],
        compiler_params=pltpu.CompilerParams(vmem_limit_bytes=STORE_BYTES),
        name="store",
    )(*arrays)


def fused(grads, weights, targets):
    rows_dev, feat_cols = grads.shape
    n_samp = lax.axis_size("samp")
    n_feat = lax.axis_size("feat")
    dirs = targets.shape[1]
    chips = n_samp // 2
    count = -(-dirs // CHUNK)
    n_direct, n_near = [len(part) for part in split_hops(chips, PART_HOPS)]
    f32, b16 = jnp.float32, jnp.bfloat16
    vmem = pl.BlockSpec(memory_space=pltpu.VMEM)
    dma = pltpu.SemaphoreType.DMA
    scores, solved, resid = pl.pallas_call(
        functools.partial(kernel, rows_dev * n_samp, feat_cols * n_feat),
        out_shape=(
            jax.ShapeDtypeStruct((dirs, rows_dev // n_feat), f32),
            jax.ShapeDtypeStruct((dirs, feat_cols), f32),
            jax.ShapeDtypeStruct((dirs, feat_cols), f32),
        ),
        in_specs=[pl.BlockSpec(memory_space=pltpu.HBM)] * 3,
        out_specs=[vmem] * 3,
        scratch_shapes=[
            pltpu.VMEM((rows_dev, feat_cols), b16),
            pltpu.VMEM((1, rows_dev), f32),
            pltpu.VMEM((dirs, feat_cols), f32),
            pltpu.VMEM((ITERS, dirs, rows_dev), b16),
            pltpu.VMEM((ITERS, dirs, rows_dev), b16),
            pltpu.VMEM((dirs, rows_dev), f32),
            pltpu.VMEM((dirs, rows_dev), f32),
            pltpu.VMEM((dirs, LANES), f32),
            pltpu.VMEM((dirs, LANES), f32),
            pltpu.VMEM((count, 8, LANES), f32),
            pltpu.VMEM((count, 8, LANES), f32),
            pltpu.VMEM((ITERS, 2, n_near, dirs, LANES), b16),
            pltpu.VMEM((ITERS, n_near, dirs, LANES), b16),
            pltpu.VMEM((n_near, dirs, LANES), f32),
            pltpu.VMEM((ITERS, max(1, n_near - 1), dirs, LANES), b16),
            pltpu.VMEM((ITERS, max(1, n_direct), 2, dirs, LANES), b16),
            pltpu.VMEM((ITERS, 2 * n_direct + n_near - 1, dirs, LANES), b16),
            pltpu.VMEM((ITERS, chips, 2, dirs, LANES), b16),
            pltpu.VMEM((count, 8, LANES), f32),
            pltpu.VMEM((count, n_samp, LANES), f32),
            dma((4,)),
            dma((ITERS, count, 2)), dma((ITERS, count, 2)),
            dma((ITERS, count)), dma((ITERS, count)),
            dma((ITERS, count)), dma((ITERS, count)),
            dma((ITERS, count)), dma((ITERS, count, chips)),
            dma((ITERS, count)), dma((ITERS, count, chips)),
            dma((count,)), dma((count,)),
        ],
        compiler_params=pltpu.CompilerParams(collective_id=0, has_side_effects=True, vmem_limit_bytes=VMEM_BYTES),
        name="cg",
    )(grads, pltpu.with_memory_space_constraint(weights[None, :], pltpu.HBM), targets.T)
    scores, solved, resid = write_out(scores, solved, resid)
    return scores.T, solved.T, resid.T


def per_device(grads, weights, targets):
    rows_dev, feat_cols = grads.shape
    n_samp = lax.axis_size("samp")
    n_feat = lax.axis_size("feat")
    total = rows_dev * n_samp
    full_width = feat_cols * n_feat
    share = rows_dev // n_feat
    offset = lax.axis_index("feat") * share
    scaled = weights / total
    regrouped = lax.all_to_all(grads, "feat", split_axis=0, concat_axis=1, tiled=True)
    own_weights = lax.dynamic_slice_in_dim(scaled, offset, share, 0)

    def column_norms(resid):
        squares = jnp.sum(resid * resid, axis=0)
        parts = (squares,)
        return lax.psum((parts[0],), "feat")

    solution = jnp.zeros_like(targets)
    resid = targets
    direction = targets
    accum = jnp.zeros((share, targets.shape[1]), jnp.float32)
    norm_now = column_norms(resid)[0]
    for step in range(ITERS):
        packed = direction.astype(jnp.bfloat16)
        sample_rows = jnp.dot(
            regrouped,
            lax.all_gather(packed, "feat", axis=0, tiled=True),
            preferred_element_type=jnp.float32,
        )
        weighted = (sample_rows * own_weights[:, None]).astype(jnp.bfloat16)
        partial_image = lax.psum_scatter(
            lax.dot_general(
                regrouped, weighted, (((0,), (0,)), ((), ())), preferred_element_type=jnp.float32
            ).astype(jnp.bfloat16),
            "feat",
            scatter_dimension=0,
            tiled=True,
        ).astype(jnp.float32)
        own_rows = sample_rows
        apply_own_weights = own_weights
        image = lax.psum(partial_image, "samp") + damping_term * direction
        own_rows, own_weights, image = (own_rows, apply_own_weights, image)
        curvature = lax.psum(jnp.sum(direction * image, axis=0), "feat")
        alpha = norm_now / curvature
        solution = solution + alpha * direction
        resid = resid - alpha * image
        accum = accum + alpha * own_rows
        if step + 1 < ITERS:
            sums = column_norms(resid)
            norm_next = sums[0]
            ratio = norm_next / norm_now
            direction = resid + ratio * direction
            norm_now = norm_next
    scores = accum / math.sqrt(full_width)
    return (scores, solution, resid)


def dispatch(grads, weights, targets):
    rows_dev, feat_cols = grads.shape
    n_samp, n_feat = lax.axis_size("samp"), lax.axis_size("feat")
    fits = (
        n_feat == 2
        and n_samp >= 4
        and n_samp & (n_samp - 1) == 0
        and feat_cols == n_samp * LANES
        and rows_dev % (2 * LANES) == 0
        and targets.shape[1] % CHUNK == 0
        and targets.shape[1] <= LANES
    )
    return (fused if fits else per_device)(grads, weights, targets)


def solution(mesh):
    return jax.shard_map(
        dispatch,
        mesh=mesh,
        in_specs=(P("samp", "feat"), P("samp"), P("feat", None)),
        out_specs=(P(("samp", "feat"), None), P("feat", None), P("feat", None)),
        check_vma=False,
    )
```

```python
import functools
import math

import jax
import jax.numpy as jnp
from jax import lax
from jax.experimental import pallas as pl
from jax.experimental.pallas import tpu as pltpu
from jax.sharding import PartitionSpec as P

ITERS = 2
CHUNK = 32
PART_HOPS = 5
TILE_HOPS = 5
EARLY_HOPS = 2
LANES = 128
VMEM_BYTES = 105 * 2**19
STORE_BYTES = 2**22
MESH = pl.DeviceIdType.MESH

damping_term = 0.1


def kernel(
    total, full_width,
    grads_hbm, weights_hbm, targets_hbm,
    scores_ref, solution_ref, resid_ref,
    grads_ref, weights_ref, targets_ref,
    rows_out, rows_in, first_rows, second_rows,
    norms_out, norms_in, sums_out, sums_in,
    swap_out, swap_in, near_f32, near_out, part_out, part_in, gathered, curve_out, curve_in,
    load_sem, x_send, x_recv, swap_send, swap_recv, part_send, part_recv,
    gather_send, gather_recv, pass_send, pass_recv, curve_send, curve_recv,
):
    samp, feat = lax.axis_index("samp"), lax.axis_index("feat")
    n_samp = curve_in.shape[1]
    chips = n_samp // 2
    core, chip = lax.rem(samp, 2), lax.div(samp, 2)
    dirs = targets_ref.shape[0]
    rows_dev = grads_ref.shape[0]
    half = rows_dev // 2
    pair = 2 * LANES
    groups = [slice(i, min(i + CHUNK, dirs)) for i in range(0, dirs, CHUNK)]
    count = len(groups)
    f32, b16 = jnp.float32, jnp.bfloat16
    nt = (((1,), (1,)), ((), ()))
    mirror = (samp, 1 - feat)

    def flipped(index, mask, bits):
        for b in range(bits):
            if (mask >> b) & 1:
                index = index + (1 - 2 * lax.rem(lax.div(index, 2**b), 2)) * 2**b
        return index

    bits = (chips - 1).bit_length()
    peer_chip = [flipped(chip, j, bits) for j in range(chips)]
    near_first = hop_order(chips)
    far_first = near_first[::-1]
    direct, near = split_hops(chips, PART_HOPS)
    wide, narrow = split_hops(chips, TILE_HOPS)
    partner = (chip * 2 + 1 - core, feat)

    def peer(j, c):
        to = core if c == 0 else 1 - core
        return to, (peer_chip[j] * 2 + to, feat)

    others = [(j, c) for j in far_first for c in (0, 1) if (j, c) != (0, 0)]

    loads = [
        pltpu.make_async_copy(targets_hbm, targets_ref, load_sem.at[0]),
        pltpu.make_async_copy(grads_hbm.at[pl.ds(0, half)], grads_ref.at[pl.ds(0, half)], load_sem.at[1]),
        pltpu.make_async_copy(grads_hbm.at[pl.ds(half, half)], grads_ref.at[pl.ds(half, half)], load_sem.at[2]),
        pltpu.make_async_copy(weights_hbm, weights_ref, load_sem.at[3]),
    ]
    for load in loads:
        load.start()

    barrier = pltpu.get_barrier_semaphore()
    for device in [mirror] + [peer(j, c)[1] for j, c in others]:
        pl.semaphore_signal(barrier, inc=1, device_id=device, device_id_type=MESH)

    def remote(src, dst, send, recv, device):
        return pltpu.make_async_remote_copy(
            src_ref=src, dst_ref=dst, send_sem=send, recv_sem=recv, device_id=device, device_id_type=MESH
        )

    def rows_of(g):
        return pl.ds(groups[g].start, groups[g].stop - groups[g].start)

    def pair_lanes(j):
        return pl.ds(pl.multiple_of(peer_chip[j] * pair, pair), pair)

    own_lanes = pl.ds(pl.multiple_of(samp * LANES, LANES), LANES)

    def x_copy(s, g, kind):
        if kind == 0:
            src, dst = rows_out.at[s, rows_of(g)], rows_in.at[s, rows_of(g)]
        elif s == 0:
            src, dst = norms_out.at[rows_of(g)], norms_in.at[rows_of(g)]
        else:
            src, dst = sums_out.at[g, pl.ds(0, 2)], sums_in.at[g, pl.ds(0, 2)]
        return remote(src, dst, x_send.at[s, g, kind], x_recv.at[s, g, kind], mirror)

    def size_of(g):
        return groups[g].stop - groups[g].start

    def swap_copy(s, g):
        return remote(
            swap_out.at[s, 1 - core, :, rows_of(g)], swap_in.at[s, :, rows_of(g)],
            swap_send.at[s, g], swap_recv.at[s, g], partner)

    def part_copy(s, g, j, c):
        to, device = peer(j, c)
        if j in near:
            place = near.index(j) - 1
            src, slot = near_out.at[s, place, rows_of(g)], 2 * len(direct) + place
        else:
            src, slot = part_out.at[s, direct.index(j), to, rows_of(g)], 2 * direct.index(j) + c
        return remote(src, part_in.at[s, slot, rows_of(g)], part_send.at[s, g], part_recv.at[s, g], device)

    def part_all(s, g):
        ref = part_in.at[s, :, rows_of(g)]
        return remote(ref, ref, part_send.at[s, g], part_recv.at[s, g], mirror)

    def tile_copy(s, g, j, c):
        to, device = peer(j, c)
        ref = gathered.at[s, chip, core, rows_of(g)]
        return remote(ref, ref, gather_send.at[s, g], gather_recv.at[s, g, j], device)

    def tile_sends(s, g):
        sends = [(j, 0) for j in far_first if j in narrow and j] + [(0, 1)]
        return [tile_copy(s, g, j, c) for j in wide for c in (0, 1)] + [tile_copy(s, g, j, c) for j, c in sends]

    def pass_copy(s, g, j):
        ref = gathered.at[s, peer_chip[j], core, rows_of(g)]
        return remote(ref, ref, pass_send.at[s, g], pass_recv.at[s, g, j], partner)

    def tile_arrival(s, g, j):
        if j == 0:
            ref = gathered.at[s, chip, 1 - core, rows_of(g)]
        elif j in narrow:
            ref = gathered.at[s, peer_chip[j], core, rows_of(g)]
        else:
            ref = gathered.at[s, peer_chip[j], pl.ds(0, 2), rows_of(g)]
        remote(ref, ref, gather_send.at[s, g], gather_recv.at[s, g, j], mirror).wait_recv()

    def tile_wait(s, g, j):
        if j == 0 or j in wide:
            tile_arrival(s, g, j)
        else:
            ref = gathered.at[s, peer_chip[j], 1 - core, rows_of(g)]
            remote(ref, ref, pass_send.at[s, g], pass_recv.at[s, g, j], partner).wait_recv()

    early = [j for j in near_first if hops(j) < EARLY_HOPS]
    parts = [early, [j for j in near_first if j not in early]]

    def forward(s, g, part):
        for j in parts[part]:
            if j in narrow and j:
                tile_arrival(s, g, j)
                pass_copy(s, g, j).start()

    def curve_copy(g, j, c):
        to, device = peer(j, c)
        return remote(
            curve_out.at[g, pl.ds(0, 1)], curve_in.at[g, pl.ds(2 * j + c, 1)],
            curve_send.at[g], curve_recv.at[g], device)

    def curve_all(g):
        ref = curve_in.at[g, pl.ds(1, n_samp - 1)]
        return remote(ref, ref, curve_send.at[g], curve_recv.at[g], mirror)

    def lane_sum(block):
        folded = block[:, :LANES]
        for i in range(1, block.shape[1] // LANES):
            folded = folded + block[:, i * LANES : (i + 1) * LANES]
        return folded

    def column(block):
        return jnp.sum(block, axis=1, keepdims=True)

    def diagonal(size):
        shape = (size, LANES)
        return lax.broadcasted_iota(jnp.int32, shape, 0) == lax.broadcasted_iota(jnp.int32, shape, 1)

    def to_line(values, size):
        return jnp.sum(jnp.where(diagonal(size), values, 0.0), axis=0, keepdims=True)

    def to_column(line, size):
        return column(jnp.where(diagonal(size), line, 0.0))

    loads[0].wait()
    targets = targets_ref[...]
    packed = targets.astype(b16)
    for h in range(2):
        part_h = slice(h * half, (h + 1) * half)
        loads[1 + h].wait()
        part = lax.dot_general(packed, grads_ref[part_h, :], nt, preferred_element_type=f32)
        first_rows[:, part_h] = part
        rows_out[0, :, part_h] = part.astype(b16)
    pl.semaphore_wait(barrier, n_samp)
    for g in range(count):
        x_copy(0, g, 0).start()
    norms_out[...] = lane_sum(targets * targets)
    for g in range(count):
        x_copy(0, g, 1).start()
    loads[3].wait()
    scaled = weights_ref[...] / total
    state = [dict() for _ in range(count)]

    def exchange(s, g):
        now, rows = state[g], groups[g]
        if s == 0:
            x_copy(0, g, 0).wait_recv()
            whole = first_rows[rows, :] + rows_in[0, rows, :].astype(f32)
            first_rows[rows, :] = whole
        else:
            x_copy(0, g, 1).wait_recv()
            x_copy(1, g, 1).wait_recv()
            norm0 = column(norms_out[rows, :] + norms_in[rows, :])
            both = sums_out[g, 0:2, :] + sums_in[g, 0:2, :]
            along, square = [to_column(both[i : i + 1], size_of(g)) for i in range(2)]
            alpha0 = norm0 / along
            cross = norm0 - alpha0 * along
            norm1 = cross - alpha0 * (along - alpha0 * square)
            ratio = norm1 / norm0
            now.update(alpha0=alpha0, norm1=norm1, ratio=ratio,
                       length=norm1 + 2.0 * ratio * cross + ratio * ratio * norm0)
            x_copy(1, g, 0).wait_recv()
            image_rows = second_rows[rows, :] + rows_in[1, rows, :].astype(f32)
            whole = (1.0 + ratio) * first_rows[rows, :] - alpha0 * image_rows
            second_rows[rows, :] = whole
        weighted = (whole * scaled).astype(b16)
        for j in far_first:
            image = jnp.dot(weighted, grads_ref[:, pair_lanes(j)], preferred_element_type=f32)
            tiles = [image[:, c * LANES : (c + 1) * LANES] for c in range(2)]
            if j in near:
                near_f32[near.index(j), rows, :] = jnp.where(core == 0, tiles[0], tiles[1])
            for c in range(2):
                if j in near:
                    swap_out[s, c, near.index(j), rows, :] = tiles[c].astype(b16)
                else:
                    part_out[s, direct.index(j), c, rows, :] = tiles[c].astype(b16)
        swap_copy(s, g).start()
        for j in direct:
            for c in range(2):
                part_copy(s, g, j, c).start()
        if s == 1:
            line = to_line(column(lane_sum(weighted.astype(f32) * whole)), size_of(g))
            curve_out[g, 0:1, :] = line
            curve_in[g, 0:1, :] = line
            for j, c in others:
                curve_copy(g, j, c).start()

    def swap(s, g):
        now, rows = state[g], groups[g]
        swap_copy(s, g).wait_recv()
        for place, j in reversed(list(enumerate(near))):
            both = near_f32[place, rows, :] + swap_in[s, place, rows, :].astype(f32)
            if j:
                near_out[s, place - 1, rows, :] = both.astype(b16)
                part_copy(s, g, j, 0).start()
            else:
                now["own"] = both

    def reduce(s, g):
        now, rows = state[g], groups[g]
        target = targets_ref[rows, own_lanes]
        if s == 1:
            curve_all(g).wait_recv()
            curve = to_column(jnp.sum(curve_in[g], axis=0, keepdims=True), size_of(g))
            now["alpha1"] = now["norm1"] / (curve + damping_term * now["length"])
            resid = target - now["alpha0"] * now["image0"]
            direction = resid + now["ratio"] * target
        else:
            direction = target
        part_all(s, g).wait_recv()
        image = now["own"] + damping_term * direction
        for k in range(part_in.shape[1]):
            image = image + part_in[s, k, rows, :].astype(f32)
        if s == 0:
            now["image0"] = image
            tile = image
        else:
            tile = resid - now["alpha1"] * image
        gathered[s, chip, core, rows, :] = tile.astype(b16)
        for copy in tile_sends(s, g):
            copy.start()

    def gather(s, g, part):
        now, rows = state[g], groups[g]
        for j in parts[part]:
            tile_wait(s, g, j)
        if s == 1:
            for j in parts[part]:
                for c in range(2):
                    lanes = pl.ds(pl.multiple_of(peer_chip[j] * pair + c * LANES, LANES), LANES)
                    resid_ref[rows, lanes] = gathered[1, peer_chip[j], c, rows, :].astype(f32)
            return
        mine, along, square = now.get("sums", (0.0, 0.0, 0.0))
        for j in parts[part]:
            block = jnp.concatenate([gathered[0, peer_chip[j], c, rows, :] for c in range(2)], axis=1)
            mine = mine + lax.dot_general(block, grads_ref[:, pair_lanes(j)], nt, preferred_element_type=f32)
            block = block.astype(f32)
            along = along + lane_sum(block * targets_ref[rows, pair_lanes(j)])
            square = square + lane_sum(block * block)
        if part == 0:
            now["sums"] = (mine, along, square)
            return
        for i, block in enumerate([along, square]):
            sums_out[g, i : i + 1, :] = to_line(column(block), size_of(g))
        x_copy(1, g, 1).start()
        rows_out[1, rows, :] = mine.astype(b16)
        x_copy(1, g, 0).start()
        second_rows[rows, :] = mine

    def finish(g):
        now, rows = state[g], groups[g]
        alpha0, alpha1 = now["alpha0"], now["alpha1"]
        share = rows_dev // 2
        scores = (alpha0 * first_rows[rows, :] + alpha1 * second_rows[rows, :]) / math.sqrt(full_width)
        scores_ref[rows, :] = jnp.where(feat == 0, scores[:, :share], scores[:, share:])
        start_part = alpha0 + alpha1 * (1.0 + now["ratio"])
        image_part = alpha1 * alpha0
        for i in range(chips):
            for c in range(2):
                lanes = slice(i * pair + c * LANES, i * pair + (c + 1) * LANES)
                solution_ref[rows, lanes] = (
                    start_part * targets_ref[rows, lanes] - image_part * gathered[0, i, c, rows, :].astype(f32))

    stages = dict(exchange=exchange, swap=swap, reduce=reduce, forward=forward, gather=gather, finish=finish)
    for step in order(count):
        stage, *where = step
        stages[stage](*where)
    for g in range(count):
        for s in range(ITERS):
            for kind in range(2):
                x_copy(s, g, kind).wait_send()
            swap_copy(s, g).wait_send()
            part_all(s, g).wait_send()
            for copy in tile_sends(s, g):
                copy.wait_send()
            for j in narrow:
                if j:
                    pass_copy(s, g, j).wait_send()
        curve_all(g).wait_send()


def hop_order(chips):
    return sorted(range(chips), key=hops)


def hops(j):
    return j // 2 + j % 2


def split_hops(chips, limit):
    ordered = hop_order(chips)
    return [j for j in ordered if hops(j) >= limit], [j for j in ordered if hops(j) < limit]


def order(count):
    every = range(count)
    steps = [(stage, 0, g) for stage in ("exchange", "swap") for g in every]
    for s in range(ITERS):
        if s == 1:
            steps += [(stage, s, g) for g in every for stage in ("exchange", "swap")]
        steps += [("reduce", s, g) for g in every]
        if s == ITERS - 1:
            steps += [("finish", g) for g in every]
        steps += [("forward", s, 0, 0), ("forward", s, 0, 1)]
        for g in every:
            if g + 1 < count:
                steps.append(("forward", s, g + 1, 0))
            steps += [("gather", s, g, 0), ("gather", s, g, 1)]
            if g + 1 < count:
                steps.append(("forward", s, g + 1, 1))
    return steps


def store_kernel(*refs):
    count = len(refs) // 2
    sem = refs[-1]
    copies = [pltpu.make_async_copy(refs[i], refs[count + i], sem.at[i]) for i in range(count)]
    for copy in copies:
        copy.start()
    for copy in copies:
        copy.wait()


def write_out(*arrays):
    return pl.pallas_call(
        store_kernel,
        out_shape=tuple(jax.ShapeDtypeStruct(a.shape, a.dtype) for a in arrays),
        in_specs=[pl.BlockSpec(memory_space=pltpu.VMEM)] * len(arrays),
        out_specs=[pl.BlockSpec(memory_space=pltpu.HBM)] * len(arrays),
        scratch_shapes=[pltpu.SemaphoreType.DMA((len(arrays),))],
        compiler_params=pltpu.CompilerParams(vmem_limit_bytes=STORE_BYTES),
        name="store",
    )(*arrays)


def fused(grads, weights, targets):
    rows_dev, feat_cols = grads.shape
    n_samp = lax.axis_size("samp")
    n_feat = lax.axis_size("feat")
    dirs = targets.shape[1]
    chips = n_samp // 2
    count = -(-dirs // CHUNK)
    n_direct, n_near = [len(part) for part in split_hops(chips, PART_HOPS)]
    f32, b16 = jnp.float32, jnp.bfloat16
    vmem = pl.BlockSpec(memory_space=pltpu.VMEM)
    dma = pltpu.SemaphoreType.DMA
    scores, solved, resid = pl.pallas_call(
        functools.partial(kernel, rows_dev * n_samp, feat_cols * n_feat),
        out_shape=(
            jax.ShapeDtypeStruct((dirs, rows_dev // n_feat), f32),
            jax.ShapeDtypeStruct((dirs, feat_cols), f32),
            jax.ShapeDtypeStruct((dirs, feat_cols), f32),
        ),
        in_specs=[pl.BlockSpec(memory_space=pltpu.HBM)] * 3,
        out_specs=[vmem] * 3,
        scratch_shapes=[
            pltpu.VMEM((rows_dev, feat_cols), b16),
            pltpu.VMEM((1, rows_dev), f32),
            pltpu.VMEM((dirs, feat_cols), f32),
            pltpu.VMEM((ITERS, dirs, rows_dev), b16),
            pltpu.VMEM((ITERS, dirs, rows_dev), b16),
            pltpu.VMEM((dirs, rows_dev), f32),
            pltpu.VMEM((dirs, rows_dev), f32),
            pltpu.VMEM((dirs, LANES), f32),
            pltpu.VMEM((dirs, LANES), f32),
            pltpu.VMEM((count, 8, LANES), f32),
            pltpu.VMEM((count, 8, LANES), f32),
            pltpu.VMEM((ITERS, 2, n_near, dirs, LANES), b16),
            pltpu.VMEM((ITERS, n_near, dirs, LANES), b16),
            pltpu.VMEM((n_near, dirs, LANES), f32),
            pltpu.VMEM((ITERS, max(1, n_near - 1), dirs, LANES), b16),
            pltpu.VMEM((ITERS, max(1, n_direct), 2, dirs, LANES), b16),
            pltpu.VMEM((ITERS, 2 * n_direct + n_near - 1, dirs, LANES), b16),
            pltpu.VMEM((ITERS, chips, 2, dirs, LANES), b16),
            pltpu.VMEM((count, 8, LANES), f32),
            pltpu.VMEM((count, n_samp, LANES), f32),
            dma((4,)),
            dma((ITERS, count, 2)), dma((ITERS, count, 2)),
            dma((ITERS, count)), dma((ITERS, count)),
            dma((ITERS, count)), dma((ITERS, count)),
            dma((ITERS, count)), dma((ITERS, count, chips)),
            dma((ITERS, count)), dma((ITERS, count, chips)),
            dma((count,)), dma((count,)),
        ],
        compiler_params=pltpu.CompilerParams(collective_id=0, has_side_effects=True, vmem_limit_bytes=VMEM_BYTES),
        name="cg",
    )(grads, pltpu.with_memory_space_constraint(weights[None, :], pltpu.HBM), targets.T)
    scores, solved, resid = write_out(scores, solved, resid)
    return scores.T, solved.T, resid.T


def per_device(grads, weights, targets):
    rows_dev, feat_cols = grads.shape
    n_samp = lax.axis_size("samp")
    n_feat = lax.axis_size("feat")
    total = rows_dev * n_samp
    full_width = feat_cols * n_feat
    share = rows_dev // n_feat
    offset = lax.axis_index("feat") * share
    scaled = weights / total
    regrouped = lax.all_to_all(grads, "feat", split_axis=0, concat_axis=1, tiled=True)
    own_weights = lax.dynamic_slice_in_dim(scaled, offset, share, 0)

    def column_norms(resid):
        squares = jnp.sum(resid * resid, axis=0)
        parts = (squares,)
        return lax.psum((parts[0],), "feat")

    solution = jnp.zeros_like(targets)
    resid = targets
    direction = targets
    accum = jnp.zeros((share, targets.shape[1]), jnp.float32)
    norm_now = column_norms(resid)[0]
    for step in range(ITERS):
        packed = direction.astype(jnp.bfloat16)
        sample_rows = jnp.dot(
            regrouped,
            lax.all_gather(packed, "feat", axis=0, tiled=True),
            preferred_element_type=jnp.float32,
        )
        weighted = (sample_rows * own_weights[:, None]).astype(jnp.bfloat16)
        partial_image = lax.psum_scatter(
            lax.dot_general(
                regrouped, weighted, (((0,), (0,)), ((), ())), preferred_element_type=jnp.float32
            ).astype(jnp.bfloat16),
            "feat",
            scatter_dimension=0,
            tiled=True,
        ).astype(jnp.float32)
        own_rows = sample_rows
        apply_own_weights = own_weights
        image = lax.psum(partial_image, "samp") + damping_term * direction
        own_rows, own_weights, image = (own_rows, apply_own_weights, image)
        curvature = lax.psum(jnp.sum(direction * image, axis=0), "feat")
        alpha = norm_now / curvature
        solution = solution + alpha * direction
        resid = resid - alpha * image
        accum = accum + alpha * own_rows
        if step + 1 < ITERS:
            sums = column_norms(resid)
            norm_next = sums[0]
            ratio = norm_next / norm_now
            direction = resid + ratio * direction
            norm_now = norm_next
    scores = accum / math.sqrt(full_width)
    return (scores, solution, resid)


def dispatch(grads, weights, targets):
    rows_dev, feat_cols = grads.shape
    n_samp, n_feat = lax.axis_size("samp"), lax.axis_size("feat")
    fits = (
        n_feat == 2
        and n_samp >= 4
        and n_samp & (n_samp - 1) == 0
        and feat_cols == n_samp * LANES
        and rows_dev % (2 * LANES) == 0
        and targets.shape[1] % CHUNK == 0
        and targets.shape[1] <= LANES
    )
    return (fused if fits else per_device)(grads, weights, targets)


def solution(mesh):
    return jax.shard_map(
        dispatch,
        mesh=mesh,
        in_specs=(P("samp", "feat"), P("samp"), P("feat", None)),
        out_specs=(P(("samp", "feat"), None), P("feat", None), P("feat", None)),
        check_vma=False,
    )
```

```python
import functools
import math

import jax
import jax.numpy as jnp
from jax import lax
from jax.experimental import pallas as pl
from jax.experimental.pallas import tpu as pltpu
from jax.sharding import PartitionSpec as P

ITERS = 2
CHUNK = 32
PIECES = 4
PART_HOPS = 5
TILE_HOPS = 5
EARLY_HOPS = 2
LANES = 128
VMEM_BYTES = 105 * 2**19
STORE_BYTES = 2**22
MESH = pl.DeviceIdType.MESH

damping_term = 0.1


def kernel(
    total, full_width,
    grads_hbm, weights_hbm, targets_hbm,
    scores_ref, solution_ref, resid_ref,
    grads_ref, weights_ref, targets_ref,
    rows_out, rows_in, first_rows, second_rows,
    norms_out, norms_in, sums_out, sums_in,
    swap_out, swap_in, near_f32, near_out, part_out, part_in, gathered, curve_out, curve_in,
    load_sem, x_send, x_recv, swap_send, swap_recv, part_send, part_recv,
    gather_send, gather_recv, pass_send, pass_recv, curve_send, curve_recv,
):
    samp, feat = lax.axis_index("samp"), lax.axis_index("feat")
    n_samp = curve_in.shape[1]
    chips = n_samp // 2
    core, chip = lax.rem(samp, 2), lax.div(samp, 2)
    dirs = targets_ref.shape[0]
    rows_dev = grads_ref.shape[0]
    pair = 2 * LANES
    groups = [slice(i, min(i + CHUNK, dirs)) for i in range(0, dirs, CHUNK)]
    count = len(groups)
    f32, b16 = jnp.float32, jnp.bfloat16
    nt = (((1,), (1,)), ((), ()))
    mirror = (samp, 1 - feat)

    def flipped(index, mask, bits):
        for b in range(bits):
            if (mask >> b) & 1:
                index = index + (1 - 2 * lax.rem(lax.div(index, 2**b), 2)) * 2**b
        return index

    bits = (chips - 1).bit_length()
    peer_chip = [flipped(chip, j, bits) for j in range(chips)]
    near_first = hop_order(chips)
    far_first = near_first[::-1]
    direct, near = split_hops(chips, PART_HOPS)
    wide, narrow = split_hops(chips, TILE_HOPS)
    partner = (chip * 2 + 1 - core, feat)
    line = lax.div(chip, 2)
    inner = lax.rem(line + lax.div(line, 2), 2)

    def nearer(j):
        return j ^ 2 if j >= chips // 2 and chips >= 8 else j

    def routed(j, value_of):
        mine, other = value_of(j), value_of(nearer(j))
        return mine if nearer(j) == j else mine + inner * (other - mine)

    def peer(j, c):
        to = core if c == 0 else 1 - core
        return to, (peer_chip[j] * 2 + to, feat)

    others = [(j, c) for j in far_first for c in (0, 1) if (j, c) != (0, 0)]

    loads = [
        pltpu.make_async_copy(targets_hbm, targets_ref, load_sem.at[0]),
        pltpu.make_async_copy(weights_hbm, weights_ref, load_sem.at[1]),
    ]
    piece = grads_ref.shape[1] // PIECES
    pieces = [pl.ds(i * piece, piece) for i in range(PIECES)]
    loads += [
        pltpu.make_async_copy(grads_hbm.at[:, lanes], grads_ref.at[:, lanes], load_sem.at[2 + i])
        for i, lanes in enumerate(pieces)
    ]
    for load in loads:
        load.start()

    barrier = pltpu.get_barrier_semaphore()
    for device in [mirror] + [peer(j, c)[1] for j, c in others]:
        pl.semaphore_signal(barrier, inc=1, device_id=device, device_id_type=MESH)

    def remote(src, dst, send, recv, device):
        return pltpu.make_async_remote_copy(
            src_ref=src, dst_ref=dst, send_sem=send, recv_sem=recv, device_id=device, device_id_type=MESH
        )

    def rows_of(g):
        return pl.ds(groups[g].start, groups[g].stop - groups[g].start)

    def pair_lanes(j):
        return pl.ds(pl.multiple_of(peer_chip[j] * pair, pair), pair)

    own_lanes = pl.ds(pl.multiple_of(samp * LANES, LANES), LANES)

    def x_copy(s, g, kind):
        if kind == 0:
            src, dst = rows_out.at[s, rows_of(g)], rows_in.at[s, rows_of(g)]
        elif s == 0:
            src, dst = norms_out.at[rows_of(g)], norms_in.at[rows_of(g)]
        else:
            src, dst = sums_out.at[g, pl.ds(0, 2)], sums_in.at[g, pl.ds(0, 2)]
        return remote(src, dst, x_send.at[s, g, kind], x_recv.at[s, g, kind], mirror)

    def size_of(g):
        return groups[g].stop - groups[g].start

    def swap_copy(s, g):
        return remote(
            swap_out.at[s, 1 - core, :, rows_of(g)], swap_in.at[s, :, rows_of(g)],
            swap_send.at[s, g], swap_recv.at[s, g], partner)

    def part_copy(s, g, j, c):
        to, device = peer(j, c)
        if j in near:
            place = near.index(j) - 1
            src, slot = near_out.at[s, place, rows_of(g)], 2 * len(direct) + place
        else:
            src, slot = part_out.at[s, direct.index(j), to, rows_of(g)], 2 * direct.index(j) + c
        return remote(src, part_in.at[s, slot, rows_of(g)], part_send.at[s, g], part_recv.at[s, g], device)

    def part_all(s, g):
        ref = part_in.at[s, :, rows_of(g)]
        return remote(ref, ref, part_send.at[s, g], part_recv.at[s, g], mirror)

    def tile_copy(s, g, j, c):
        to, device = peer(j, c)
        ref = gathered.at[s, chip, core, rows_of(g)]
        return remote(ref, ref, gather_send.at[s, g], gather_recv.at[s, g, j], device)

    def far_tile_copy(s, g, j):
        ref = gathered.at[s, chip, core, rows_of(g)]
        device = (routed(j, lambda i: peer_chip[i]) * 2 + core, feat)
        return remote(ref, ref, gather_send.at[s, g], gather_recv.at[s, g, routed(j, lambda i: i)], device)

    def far_part_copy(s, g, j):
        place = routed(j, lambda i: near.index(i) - 1)
        device = (routed(j, lambda i: peer_chip[i]) * 2 + core, feat)
        return remote(
            near_out.at[s, place, rows_of(g)], part_in.at[s, place, rows_of(g)],
            part_send.at[s, g], part_recv.at[s, g], device)

    def tile_sends(s, g):
        return [far_tile_copy(s, g, j) for j in far_first if j] + [tile_copy(s, g, 0, 1)]

    def pass_copy(s, g, j):
        ref = gathered.at[s, peer_chip[j], core, rows_of(g)]
        return remote(ref, ref, pass_send.at[s, g], pass_recv.at[s, g, j], partner)

    def tile_arrival(s, g, j):
        if j == 0:
            ref = gathered.at[s, chip, 1 - core, rows_of(g)]
        elif j in narrow:
            ref = gathered.at[s, peer_chip[j], core, rows_of(g)]
        else:
            ref = gathered.at[s, peer_chip[j], pl.ds(0, 2), rows_of(g)]
        remote(ref, ref, gather_send.at[s, g], gather_recv.at[s, g, j], mirror).wait_recv()

    def tile_wait(s, g, j):
        if j == 0 or j in wide:
            tile_arrival(s, g, j)
        else:
            ref = gathered.at[s, peer_chip[j], 1 - core, rows_of(g)]
            remote(ref, ref, pass_send.at[s, g], pass_recv.at[s, g, j], partner).wait_recv()

    early = [j for j in near_first if hops(j) < EARLY_HOPS]
    parts = [early, [j for j in near_first if j not in early]]

    def forward(s, g, part):
        for j in parts[part]:
            if j in narrow and j:
                tile_arrival(s, g, j)
                pass_copy(s, g, j).start()

    def curve_copy(g, j, c):
        to, device = peer(j, c)
        return remote(
            curve_out.at[g, pl.ds(0, 1)], curve_in.at[g, pl.ds(2 * j + c, 1)],
            curve_send.at[g], curve_recv.at[g], device)

    def curve_all(g):
        ref = curve_in.at[g, pl.ds(1, n_samp - 1)]
        return remote(ref, ref, curve_send.at[g], curve_recv.at[g], mirror)

    def lane_sum(block):
        folded = block[:, :LANES]
        for i in range(1, block.shape[1] // LANES):
            folded = folded + block[:, i * LANES : (i + 1) * LANES]
        return folded

    def column(block):
        return jnp.sum(block, axis=1, keepdims=True)

    def diagonal(size):
        shape = (size, LANES)
        return lax.broadcasted_iota(jnp.int32, shape, 0) == lax.broadcasted_iota(jnp.int32, shape, 1)

    def to_line(values, size):
        return jnp.sum(jnp.where(diagonal(size), values, 0.0), axis=0, keepdims=True)

    def to_column(line, size):
        return column(jnp.where(diagonal(size), line, 0.0))

    loads[0].wait()
    targets = targets_ref[...]
    packed = targets.astype(b16)
    part = 0.0
    for i, lanes in enumerate(pieces):
        loads[2 + i].wait()
        part = part + lax.dot_general(
            packed[:, i * piece : (i + 1) * piece], grads_ref[:, lanes], nt, preferred_element_type=f32)
    first_rows[...] = part
    rows_out[0] = part.astype(b16)
    pl.semaphore_wait(barrier, n_samp)
    for g in range(count):
        x_copy(0, g, 0).start()
    norms_out[...] = lane_sum(targets * targets)
    for g in range(count):
        x_copy(0, g, 1).start()
    loads[1].wait()
    scaled = weights_ref[...] / total
    state = [dict() for _ in range(count)]

    def exchange(s, g):
        now, rows = state[g], groups[g]
        if s == 0:
            x_copy(0, g, 0).wait_recv()
            whole = first_rows[rows, :] + rows_in[0, rows, :].astype(f32)
            first_rows[rows, :] = whole
        else:
            x_copy(0, g, 1).wait_recv()
            x_copy(1, g, 1).wait_recv()
            norm0 = column(norms_out[rows, :] + norms_in[rows, :])
            both = sums_out[g, 0:2, :] + sums_in[g, 0:2, :]
            along, square = [to_column(both[i : i + 1], size_of(g)) for i in range(2)]
            alpha0 = norm0 / along
            cross = norm0 - alpha0 * along
            norm1 = cross - alpha0 * (along - alpha0 * square)
            ratio = norm1 / norm0
            now.update(alpha0=alpha0, norm1=norm1, ratio=ratio,
                       length=norm1 + 2.0 * ratio * cross + ratio * ratio * norm0)
            x_copy(1, g, 0).wait_recv()
            image_rows = second_rows[rows, :] + rows_in[1, rows, :].astype(f32)
            whole = (1.0 + ratio) * first_rows[rows, :] - alpha0 * image_rows
            second_rows[rows, :] = whole
        weighted = (whole * scaled).astype(b16)
        for j in far_first:
            image = jnp.dot(weighted, grads_ref[:, pair_lanes(j)], preferred_element_type=f32)
            tiles = [image[:, c * LANES : (c + 1) * LANES] for c in range(2)]
            if j in near:
                near_f32[near.index(j), rows, :] = jnp.where(core == 0, tiles[0], tiles[1])
            for c in range(2):
                if j in near:
                    swap_out[s, c, near.index(j), rows, :] = tiles[c].astype(b16)
                else:
                    part_out[s, direct.index(j), c, rows, :] = tiles[c].astype(b16)
        swap_copy(s, g).start()
        for j in direct:
            for c in range(2):
                part_copy(s, g, j, c).start()
        if s == 1:
            line = to_line(column(lane_sum(weighted.astype(f32) * whole)), size_of(g))
            curve_out[g, 0:1, :] = line
            curve_in[g, 0:1, :] = line
            for j, c in others:
                curve_copy(g, j, c).start()

    def swap(s, g):
        now, rows = state[g], groups[g]
        swap_copy(s, g).wait_recv()
        for place, j in reversed(list(enumerate(near))):
            both = near_f32[place, rows, :] + swap_in[s, place, rows, :].astype(f32)
            if j == 0:
                now["own"] = both
                continue
            near_out[s, place - 1, rows, :] = both.astype(b16)
            if nearer(j) == j:
                far_part_copy(s, g, j).start()
            elif j == chips // 2:
                for i in far_first:
                    if nearer(i) != i:
                        far_part_copy(s, g, i).start()

    def reduce(s, g):
        now, rows = state[g], groups[g]
        target = targets_ref[rows, own_lanes]
        if s == 1:
            curve_all(g).wait_recv()
            curve = to_column(jnp.sum(curve_in[g], axis=0, keepdims=True), size_of(g))
            now["alpha1"] = now["norm1"] / (curve + damping_term * now["length"])
            resid = target - now["alpha0"] * now["image0"]
            direction = resid + now["ratio"] * target
        else:
            direction = target
        part_all(s, g).wait_recv()
        image = now["own"] + damping_term * direction
        for k in range(part_in.shape[1]):
            image = image + part_in[s, k, rows, :].astype(f32)
        if s == 0:
            now["image0"] = image
            tile = image
        else:
            tile = resid - now["alpha1"] * image
        gathered[s, chip, core, rows, :] = tile.astype(b16)
        for copy in tile_sends(s, g):
            copy.start()

    def gather(s, g, part):
        now, rows = state[g], groups[g]
        for j in parts[part]:
            tile_wait(s, g, j)
        if s == 1:
            for j in parts[part]:
                for c in range(2):
                    lanes = pl.ds(pl.multiple_of(peer_chip[j] * pair + c * LANES, LANES), LANES)
                    resid_ref[rows, lanes] = gathered[1, peer_chip[j], c, rows, :].astype(f32)
            return
        mine, along, square = now.get("sums", (0.0, 0.0, 0.0))
        for j in parts[part]:
            block = jnp.concatenate([gathered[0, peer_chip[j], c, rows, :] for c in range(2)], axis=1)
            mine = mine + lax.dot_general(block, grads_ref[:, pair_lanes(j)], nt, preferred_element_type=f32)
            block = block.astype(f32)
            along = along + lane_sum(block * targets_ref[rows, pair_lanes(j)])
            square = square + lane_sum(block * block)
        if part == 0:
            now["sums"] = (mine, along, square)
            return
        for i, block in enumerate([along, square]):
            sums_out[g, i : i + 1, :] = to_line(column(block), size_of(g))
        x_copy(1, g, 1).start()
        rows_out[1, rows, :] = mine.astype(b16)
        x_copy(1, g, 0).start()
        second_rows[rows, :] = mine

    def finish(g):
        now, rows = state[g], groups[g]
        alpha0, alpha1 = now["alpha0"], now["alpha1"]
        share = rows_dev // 2
        scores = (alpha0 * first_rows[rows, :] + alpha1 * second_rows[rows, :]) / math.sqrt(full_width)
        scores_ref[rows, :] = jnp.where(feat == 0, scores[:, :share], scores[:, share:])
        start_part = alpha0 + alpha1 * (1.0 + now["ratio"])
        image_part = alpha1 * alpha0
        for i in range(chips):
            for c in range(2):
                lanes = slice(i * pair + c * LANES, i * pair + (c + 1) * LANES)
                solution_ref[rows, lanes] = (
                    start_part * targets_ref[rows, lanes] - image_part * gathered[0, i, c, rows, :].astype(f32))

    stages = dict(exchange=exchange, swap=swap, reduce=reduce, forward=forward, gather=gather, finish=finish)
    for step in order(count):
        stage, *where = step
        stages[stage](*where)
    for g in range(count):
        for s in range(ITERS):
            for kind in range(2):
                x_copy(s, g, kind).wait_send()
            swap_copy(s, g).wait_send()
            part_all(s, g).wait_send()
            for copy in tile_sends(s, g):
                copy.wait_send()
            for j in narrow:
                if j:
                    pass_copy(s, g, j).wait_send()
        curve_all(g).wait_send()


def hop_order(chips):
    return sorted(range(chips), key=hops)


def hops(j):
    return j // 2 + j % 2


def split_hops(chips, limit):
    ordered = hop_order(chips)
    return [j for j in ordered if hops(j) >= limit], [j for j in ordered if hops(j) < limit]


def order(count):
    every = range(count)
    steps = [(stage, 0, g) for stage in ("exchange", "swap") for g in every]
    for s in range(ITERS):
        if s == 1:
            steps += [(stage, s, g) for g in every for stage in ("exchange", "swap")]
        steps += [("reduce", s, g) for g in every]
        if s == ITERS - 1:
            steps += [("finish", g) for g in every]
        steps += [("forward", s, 0, 0), ("forward", s, 0, 1)]
        for g in every:
            if g + 1 < count:
                steps.append(("forward", s, g + 1, 0))
            steps += [("gather", s, g, 0), ("gather", s, g, 1)]
            if g + 1 < count:
                steps.append(("forward", s, g + 1, 1))
    return steps


def store_kernel(*refs):
    count = len(refs) // 2
    sem = refs[-1]
    copies = [pltpu.make_async_copy(refs[i], refs[count + i], sem.at[i]) for i in range(count)]
    for copy in copies:
        copy.start()
    for copy in copies:
        copy.wait()


def write_out(*arrays):
    return pl.pallas_call(
        store_kernel,
        out_shape=tuple(jax.ShapeDtypeStruct(a.shape, a.dtype) for a in arrays),
        in_specs=[pl.BlockSpec(memory_space=pltpu.VMEM)] * len(arrays),
        out_specs=[pl.BlockSpec(memory_space=pltpu.HBM)] * len(arrays),
        scratch_shapes=[pltpu.SemaphoreType.DMA((len(arrays),))],
        compiler_params=pltpu.CompilerParams(vmem_limit_bytes=STORE_BYTES),
        name="store",
    )(*arrays)


def fused(grads, weights, targets):
    rows_dev, feat_cols = grads.shape
    n_samp = lax.axis_size("samp")
    n_feat = lax.axis_size("feat")
    dirs = targets.shape[1]
    chips = n_samp // 2
    count = -(-dirs // CHUNK)
    n_direct, n_near = [len(part) for part in split_hops(chips, PART_HOPS)]
    f32, b16 = jnp.float32, jnp.bfloat16
    vmem = pl.BlockSpec(memory_space=pltpu.VMEM)
    dma = pltpu.SemaphoreType.DMA
    scores, solved, resid = pl.pallas_call(
        functools.partial(kernel, rows_dev * n_samp, feat_cols * n_feat),
        out_shape=(
            jax.ShapeDtypeStruct((dirs, rows_dev // n_feat), f32),
            jax.ShapeDtypeStruct((dirs, feat_cols), f32),
            jax.ShapeDtypeStruct((dirs, feat_cols), f32),
        ),
        in_specs=[pl.BlockSpec(memory_space=pltpu.HBM)] * 3,
        out_specs=[vmem] * 3,
        scratch_shapes=[
            pltpu.VMEM((rows_dev, feat_cols), b16),
            pltpu.VMEM((1, rows_dev), f32),
            pltpu.VMEM((dirs, feat_cols), f32),
            pltpu.VMEM((ITERS, dirs, rows_dev), b16),
            pltpu.VMEM((ITERS, dirs, rows_dev), b16),
            pltpu.VMEM((dirs, rows_dev), f32),
            pltpu.VMEM((dirs, rows_dev), f32),
            pltpu.VMEM((dirs, LANES), f32),
            pltpu.VMEM((dirs, LANES), f32),
            pltpu.VMEM((count, 8, LANES), f32),
            pltpu.VMEM((count, 8, LANES), f32),
            pltpu.VMEM((ITERS, 2, n_near, dirs, LANES), b16),
            pltpu.VMEM((ITERS, n_near, dirs, LANES), b16),
            pltpu.VMEM((n_near, dirs, LANES), f32),
            pltpu.VMEM((ITERS, max(1, n_near - 1), dirs, LANES), b16),
            pltpu.VMEM((ITERS, max(1, n_direct), 2, dirs, LANES), b16),
            pltpu.VMEM((ITERS, 2 * n_direct + n_near - 1, dirs, LANES), b16),
            pltpu.VMEM((ITERS, chips, 2, dirs, LANES), b16),
            pltpu.VMEM((count, 8, LANES), f32),
            pltpu.VMEM((count, n_samp, LANES), f32),
            dma((2 + PIECES,)),
            dma((ITERS, count, 2)), dma((ITERS, count, 2)),
            dma((ITERS, count)), dma((ITERS, count)),
            dma((ITERS, count)), dma((ITERS, count)),
            dma((ITERS, count)), dma((ITERS, count, chips)),
            dma((ITERS, count)), dma((ITERS, count, chips)),
            dma((count,)), dma((count,)),
        ],
        compiler_params=pltpu.CompilerParams(
            collective_id=0, has_side_effects=True, vmem_limit_bytes=VMEM_BYTES),
        name="cg",
    )(grads, pltpu.with_memory_space_constraint(weights[None, :], pltpu.HBM), targets.T)
    scores, solved, resid = write_out(scores, solved, resid)
    return scores.T, solved.T, resid.T


def per_device(grads, weights, targets):
    rows_dev, feat_cols = grads.shape
    n_samp = lax.axis_size("samp")
    n_feat = lax.axis_size("feat")
    total = rows_dev * n_samp
    full_width = feat_cols * n_feat
    share = rows_dev // n_feat
    offset = lax.axis_index("feat") * share
    scaled = weights / total
    regrouped = lax.all_to_all(grads, "feat", split_axis=0, concat_axis=1, tiled=True)
    own_weights = lax.dynamic_slice_in_dim(scaled, offset, share, 0)

    def column_norms(resid):
        squares = jnp.sum(resid * resid, axis=0)
        parts = (squares,)
        return lax.psum((parts[0],), "feat")

    solution = jnp.zeros_like(targets)
    resid = targets
    direction = targets
    accum = jnp.zeros((share, targets.shape[1]), jnp.float32)
    norm_now = column_norms(resid)[0]
    for step in range(ITERS):
        packed = direction.astype(jnp.bfloat16)
        sample_rows = jnp.dot(
            regrouped,
            lax.all_gather(packed, "feat", axis=0, tiled=True),
            preferred_element_type=jnp.float32,
        )
        weighted = (sample_rows * own_weights[:, None]).astype(jnp.bfloat16)
        partial_image = lax.psum_scatter(
            lax.dot_general(
                regrouped, weighted, (((0,), (0,)), ((), ())), preferred_element_type=jnp.float32
            ).astype(jnp.bfloat16),
            "feat",
            scatter_dimension=0,
            tiled=True,
        ).astype(jnp.float32)
        own_rows = sample_rows
        apply_own_weights = own_weights
        image = lax.psum(partial_image, "samp") + damping_term * direction
        own_rows, own_weights, image = (own_rows, apply_own_weights, image)
        curvature = lax.psum(jnp.sum(direction * image, axis=0), "feat")
        alpha = norm_now / curvature
        solution = solution + alpha * direction
        resid = resid - alpha * image
        accum = accum + alpha * own_rows
        if step + 1 < ITERS:
            sums = column_norms(resid)
            norm_next = sums[0]
            ratio = norm_next / norm_now
            direction = resid + ratio * direction
            norm_now = norm_next
    scores = accum / math.sqrt(full_width)
    return (scores, solution, resid)


def dispatch(grads, weights, targets):
    rows_dev, feat_cols = grads.shape
    n_samp, n_feat = lax.axis_size("samp"), lax.axis_size("feat")
    fits = (
        n_feat == 2
        and n_samp >= 4
        and n_samp & (n_samp - 1) == 0
        and feat_cols == n_samp * LANES
        and rows_dev % (2 * LANES) == 0
        and targets.shape[1] % CHUNK == 0
        and targets.shape[1] <= LANES
    )
    return (fused if fits else per_device)(grads, weights, targets)


def solution(mesh):
    return jax.shard_map(
        dispatch,
        mesh=mesh,
        in_specs=(P("samp", "feat"), P("samp"), P("feat", None)),
        out_specs=(P(("samp", "feat"), None), P("feat", None), P("feat", None)),
        check_vma=False,
    )
```

```python
import functools
import math

import jax
import jax.numpy as jnp
from jax import lax
from jax.experimental import pallas as pl
from jax.experimental.pallas import tpu as pltpu
from jax.sharding import PartitionSpec as P

ITERS = 2
CHUNK = 32
PIECES = 4
PART_HOPS = 5
TILE_HOPS = 5
EARLY_HOPS = 2
LANES = 128
VMEM_BYTES = 105 * 2**19
STORE_BYTES = 2**22
STORE_PIECES = 2
MESH = pl.DeviceIdType.MESH

damping_term = 0.1


def kernel(
    total, full_width,
    grads_hbm, weights_hbm, targets_hbm,
    scores_ref, solution_ref, resid_ref,
    grads_ref, weights_ref, targets_ref,
    rows_out, rows_in, first_rows, second_rows,
    norms_out, norms_in, sums_out, sums_in,
    swap_out, swap_in, near_f32, near_out, part_out, part_in, gathered, curve_out, curve_in,
    load_sem, x_send, x_recv, swap_send, swap_recv, part_send, part_recv,
    gather_send, gather_recv, pass_send, pass_recv, curve_send, curve_recv,
):
    samp, feat = lax.axis_index("samp"), lax.axis_index("feat")
    n_samp = curve_in.shape[1]
    chips = n_samp // 2
    core, chip = lax.rem(samp, 2), lax.div(samp, 2)
    dirs = targets_ref.shape[0]
    rows_dev = grads_ref.shape[0]
    pair = 2 * LANES
    groups = [slice(i, min(i + CHUNK, dirs)) for i in range(0, dirs, CHUNK)]
    count = len(groups)
    f32, b16 = jnp.float32, jnp.bfloat16
    nt = (((1,), (1,)), ((), ()))
    mirror = (samp, 1 - feat)

    def flipped(index, mask, bits):
        for b in range(bits):
            if (mask >> b) & 1:
                index = index + (1 - 2 * lax.rem(lax.div(index, 2**b), 2)) * 2**b
        return index

    bits = (chips - 1).bit_length()
    peer_chip = [flipped(chip, j, bits) for j in range(chips)]
    near_first = hop_order(chips)
    far_first = near_first[::-1]
    direct, near = split_hops(chips, PART_HOPS)
    wide, narrow = split_hops(chips, TILE_HOPS)
    partner = (chip * 2 + 1 - core, feat)
    line = lax.div(chip, 2)
    inner = lax.rem(line + lax.div(line, 2), 2)

    def nearer(j):
        return j ^ 2 if j >= chips // 2 and chips >= 8 else j

    def routed(j, value_of):
        mine, other = value_of(j), value_of(nearer(j))
        return mine if nearer(j) == j else mine + inner * (other - mine)

    def peer(j, c):
        to = core if c == 0 else 1 - core
        return to, (peer_chip[j] * 2 + to, feat)

    others = [(j, c) for j in far_first for c in (0, 1) if (j, c) != (0, 0)]

    loads = [
        pltpu.make_async_copy(targets_hbm, targets_ref, load_sem.at[0]),
        pltpu.make_async_copy(weights_hbm, weights_ref, load_sem.at[1]),
    ]
    piece = grads_ref.shape[1] // PIECES
    pieces = [pl.ds(i * piece, piece) for i in range(PIECES)]
    loads += [
        pltpu.make_async_copy(grads_hbm.at[:, lanes], grads_ref.at[:, lanes], load_sem.at[2 + i])
        for i, lanes in enumerate(pieces)
    ]
    for load in loads:
        load.start()

    barrier = pltpu.get_barrier_semaphore()
    for device in [mirror] + [peer(j, c)[1] for j, c in others]:
        pl.semaphore_signal(barrier, inc=1, device_id=device, device_id_type=MESH)

    def remote(src, dst, send, recv, device):
        return pltpu.make_async_remote_copy(
            src_ref=src, dst_ref=dst, send_sem=send, recv_sem=recv, device_id=device, device_id_type=MESH
        )

    def rows_of(g):
        return pl.ds(groups[g].start, groups[g].stop - groups[g].start)

    def pair_lanes(j):
        return pl.ds(pl.multiple_of(peer_chip[j] * pair, pair), pair)

    own_lanes = pl.ds(pl.multiple_of(samp * LANES, LANES), LANES)

    def x_copy(s, g, kind):
        if kind == 0:
            src, dst = rows_out.at[s, rows_of(g)], rows_in.at[s, rows_of(g)]
        elif s == 0:
            src, dst = norms_out.at[rows_of(g)], norms_in.at[rows_of(g)]
        else:
            src, dst = sums_out.at[g, pl.ds(0, 2)], sums_in.at[g, pl.ds(0, 2)]
        return remote(src, dst, x_send.at[s, g, kind], x_recv.at[s, g, kind], mirror)

    def size_of(g):
        return groups[g].stop - groups[g].start

    def swap_copy(s, g):
        return remote(
            swap_out.at[s, 1 - core, :, rows_of(g)], swap_in.at[s, :, rows_of(g)],
            swap_send.at[s, g], swap_recv.at[s, g], partner)

    def part_copy(s, g, j, c):
        to, device = peer(j, c)
        if j in near:
            place = near.index(j) - 1
            src, slot = near_out.at[s, place, rows_of(g)], 2 * len(direct) + place
        else:
            src, slot = part_out.at[s, direct.index(j), to, rows_of(g)], 2 * direct.index(j) + c
        return remote(src, part_in.at[s, slot, rows_of(g)], part_send.at[s, g], part_recv.at[s, g], device)

    def part_all(s, g):
        ref = part_in.at[s, :, rows_of(g)]
        return remote(ref, ref, part_send.at[s, g], part_recv.at[s, g], mirror)

    def tile_copy(s, g, j, c):
        to, device = peer(j, c)
        ref = gathered.at[s, chip, core, rows_of(g)]
        return remote(ref, ref, gather_send.at[s, g], gather_recv.at[s, g, j], device)

    def far_tile_copy(s, g, j):
        ref = gathered.at[s, chip, core, rows_of(g)]
        device = (routed(j, lambda i: peer_chip[i]) * 2 + core, feat)
        return remote(ref, ref, gather_send.at[s, g], gather_recv.at[s, g, routed(j, lambda i: i)], device)

    def far_part_copy(s, g, j):
        place = routed(j, lambda i: near.index(i) - 1)
        device = (routed(j, lambda i: peer_chip[i]) * 2 + core, feat)
        return remote(
            near_out.at[s, place, rows_of(g)], part_in.at[s, place, rows_of(g)],
            part_send.at[s, g], part_recv.at[s, g], device)

    def tile_sends(s, g):
        return [far_tile_copy(s, g, j) for j in far_first if j] + [tile_copy(s, g, 0, 1)]

    def pass_copy(s, g, j):
        ref = gathered.at[s, peer_chip[j], core, rows_of(g)]
        return remote(ref, ref, pass_send.at[s, g], pass_recv.at[s, g, j], partner)

    def tile_arrival(s, g, j):
        if j == 0:
            ref = gathered.at[s, chip, 1 - core, rows_of(g)]
        elif j in narrow:
            ref = gathered.at[s, peer_chip[j], core, rows_of(g)]
        else:
            ref = gathered.at[s, peer_chip[j], pl.ds(0, 2), rows_of(g)]
        remote(ref, ref, gather_send.at[s, g], gather_recv.at[s, g, j], mirror).wait_recv()

    def tile_wait(s, g, j):
        if j == 0 or j in wide:
            tile_arrival(s, g, j)
        else:
            ref = gathered.at[s, peer_chip[j], 1 - core, rows_of(g)]
            remote(ref, ref, pass_send.at[s, g], pass_recv.at[s, g, j], partner).wait_recv()

    early = [j for j in near_first if hops(j) < EARLY_HOPS]
    parts = [early, [j for j in near_first if j not in early]]

    def forward(s, g, part):
        for j in parts[part]:
            if j in narrow and j:
                tile_arrival(s, g, j)
                pass_copy(s, g, j).start()

    def curve_copy(g, j, c):
        to, device = peer(j, c)
        return remote(
            curve_out.at[g, pl.ds(0, 1)], curve_in.at[g, pl.ds(2 * j + c, 1)],
            curve_send.at[g], curve_recv.at[g], device)

    def curve_all(g):
        ref = curve_in.at[g, pl.ds(1, n_samp - 1)]
        return remote(ref, ref, curve_send.at[g], curve_recv.at[g], mirror)

    def lane_sum(block):
        folded = block[:, :LANES]
        for i in range(1, block.shape[1] // LANES):
            folded = folded + block[:, i * LANES : (i + 1) * LANES]
        return folded

    def column(block):
        return jnp.sum(block, axis=1, keepdims=True)

    def diagonal(size):
        shape = (size, LANES)
        return lax.broadcasted_iota(jnp.int32, shape, 0) == lax.broadcasted_iota(jnp.int32, shape, 1)

    def to_line(values, size):
        return jnp.sum(jnp.where(diagonal(size), values, 0.0), axis=0, keepdims=True)

    def to_column(line, size):
        return column(jnp.where(diagonal(size), line, 0.0))

    loads[0].wait()
    targets = targets_ref[...]
    packed = targets.astype(b16)
    part = 0.0
    for i, lanes in enumerate(pieces):
        loads[2 + i].wait()
        part = part + lax.dot_general(
            packed[:, i * piece : (i + 1) * piece], grads_ref[:, lanes], nt, preferred_element_type=f32)
    first_rows[...] = part
    rows_out[0] = part.astype(b16)
    pl.semaphore_wait(barrier, n_samp)
    for g in range(count):
        x_copy(0, g, 0).start()
    norms_out[...] = lane_sum(targets * targets)
    for g in range(count):
        x_copy(0, g, 1).start()
    loads[1].wait()
    scaled = weights_ref[...] / total
    state = [dict() for _ in range(count)]

    def exchange(s, g):
        now, rows = state[g], groups[g]
        if s == 0:
            x_copy(0, g, 0).wait_recv()
            whole = first_rows[rows, :] + rows_in[0, rows, :].astype(f32)
            first_rows[rows, :] = whole
        else:
            x_copy(0, g, 1).wait_recv()
            x_copy(1, g, 1).wait_recv()
            norm0 = column(norms_out[rows, :] + norms_in[rows, :])
            both = sums_out[g, 0:2, :] + sums_in[g, 0:2, :]
            along, square = [to_column(both[i : i + 1], size_of(g)) for i in range(2)]
            alpha0 = norm0 / along
            cross = norm0 - alpha0 * along
            norm1 = cross - alpha0 * (along - alpha0 * square)
            ratio = norm1 / norm0
            now.update(alpha0=alpha0, norm1=norm1, ratio=ratio,
                       length=norm1 + 2.0 * ratio * cross + ratio * ratio * norm0)
            x_copy(1, g, 0).wait_recv()
            image_rows = second_rows[rows, :] + rows_in[1, rows, :].astype(f32)
            whole = (1.0 + ratio) * first_rows[rows, :] - alpha0 * image_rows
            second_rows[rows, :] = whole
        weighted = (whole * scaled).astype(b16)
        for j in far_first:
            image = jnp.dot(weighted, grads_ref[:, pair_lanes(j)], preferred_element_type=f32)
            tiles = [image[:, c * LANES : (c + 1) * LANES] for c in range(2)]
            if j in near:
                near_f32[near.index(j), rows, :] = jnp.where(core == 0, tiles[0], tiles[1])
            for c in range(2):
                if j in near:
                    swap_out[s, c, near.index(j), rows, :] = tiles[c].astype(b16)
                else:
                    part_out[s, direct.index(j), c, rows, :] = tiles[c].astype(b16)
        swap_copy(s, g).start()
        for j in direct:
            for c in range(2):
                part_copy(s, g, j, c).start()
        if s == 1:
            line = to_line(column(lane_sum(weighted.astype(f32) * whole)), size_of(g))
            curve_out[g, 0:1, :] = line
            curve_in[g, 0:1, :] = line
            for j, c in others:
                curve_copy(g, j, c).start()

    def swap(s, g):
        now, rows = state[g], groups[g]
        swap_copy(s, g).wait_recv()
        for place, j in reversed(list(enumerate(near))):
            both = near_f32[place, rows, :] + swap_in[s, place, rows, :].astype(f32)
            if j == 0:
                now["own"] = both
                continue
            near_out[s, place - 1, rows, :] = both.astype(b16)
            if nearer(j) == j:
                far_part_copy(s, g, j).start()
            elif j == chips // 2:
                for i in far_first:
                    if nearer(i) != i:
                        far_part_copy(s, g, i).start()

    def reduce(s, g):
        now, rows = state[g], groups[g]
        target = targets_ref[rows, own_lanes]
        if s == 1:
            curve_all(g).wait_recv()
            curve = to_column(jnp.sum(curve_in[g], axis=0, keepdims=True), size_of(g))
            now["alpha1"] = now["norm1"] / (curve + damping_term * now["length"])
            resid = target - now["alpha0"] * now["image0"]
            direction = resid + now["ratio"] * target
        else:
            direction = target
        part_all(s, g).wait_recv()
        image = now["own"] + damping_term * direction
        for k in range(part_in.shape[1]):
            image = image + part_in[s, k, rows, :].astype(f32)
        if s == 0:
            now["image0"] = image
            tile = image
        else:
            tile = resid - now["alpha1"] * image
        gathered[s, chip, core, rows, :] = tile.astype(b16)
        for copy in tile_sends(s, g):
            copy.start()

    def gather(s, g, part):
        now, rows = state[g], groups[g]
        for j in parts[part]:
            tile_wait(s, g, j)
        if s == 1:
            for j in parts[part]:
                for c in range(2):
                    lanes = pl.ds(pl.multiple_of(peer_chip[j] * pair + c * LANES, LANES), LANES)
                    resid_ref[rows, lanes] = gathered[1, peer_chip[j], c, rows, :].astype(f32)
            return
        mine, along, square = now.get("sums", (0.0, 0.0, 0.0))
        for j in parts[part]:
            block = jnp.concatenate([gathered[0, peer_chip[j], c, rows, :] for c in range(2)], axis=1)
            mine = mine + lax.dot_general(block, grads_ref[:, pair_lanes(j)], nt, preferred_element_type=f32)
            block = block.astype(f32)
            along = along + lane_sum(block * targets_ref[rows, pair_lanes(j)])
            square = square + lane_sum(block * block)
        if part == 0:
            now["sums"] = (mine, along, square)
            return
        for i, block in enumerate([along, square]):
            sums_out[g, i : i + 1, :] = to_line(column(block), size_of(g))
        x_copy(1, g, 1).start()
        rows_out[1, rows, :] = mine.astype(b16)
        x_copy(1, g, 0).start()
        second_rows[rows, :] = mine

    def finish(g):
        now, rows = state[g], groups[g]
        alpha0, alpha1 = now["alpha0"], now["alpha1"]
        share = rows_dev // 2
        scores = (alpha0 * first_rows[rows, :] + alpha1 * second_rows[rows, :]) / math.sqrt(full_width)
        scores_ref[rows, :] = jnp.where(feat == 0, scores[:, :share], scores[:, share:])
        start_part = alpha0 + alpha1 * (1.0 + now["ratio"])
        image_part = alpha1 * alpha0
        for i in range(chips):
            for c in range(2):
                lanes = slice(i * pair + c * LANES, i * pair + (c + 1) * LANES)
                solution_ref[rows, lanes] = (
                    start_part * targets_ref[rows, lanes] - image_part * gathered[0, i, c, rows, :].astype(f32))

    stages = dict(exchange=exchange, swap=swap, reduce=reduce, forward=forward, gather=gather, finish=finish)
    for step in order(count):
        stage, *where = step
        stages[stage](*where)
    for g in range(count):
        for s in range(ITERS):
            for kind in range(2):
                x_copy(s, g, kind).wait_send()
            swap_copy(s, g).wait_send()
            part_all(s, g).wait_send()
            for copy in tile_sends(s, g):
                copy.wait_send()
            for j in narrow:
                if j:
                    pass_copy(s, g, j).wait_send()
        curve_all(g).wait_send()


def hop_order(chips):
    return sorted(range(chips), key=hops)


def hops(j):
    return j // 2 + j % 2


def split_hops(chips, limit):
    ordered = hop_order(chips)
    return [j for j in ordered if hops(j) >= limit], [j for j in ordered if hops(j) < limit]


def order(count):
    every = range(count)
    steps = [(stage, 0, g) for stage in ("exchange", "swap") for g in every]
    for s in range(ITERS):
        if s == 1:
            steps += [(stage, s, g) for g in every for stage in ("exchange", "swap")]
        steps += [("reduce", s, g) for g in every]
        if s == ITERS - 1:
            steps += [("finish", g) for g in every]
        steps += [("forward", s, 0, 0), ("forward", s, 0, 1)]
        for g in every:
            if g + 1 < count:
                steps.append(("forward", s, g + 1, 0))
            steps += [("gather", s, g, 0), ("gather", s, g, 1)]
            if g + 1 < count:
                steps.append(("forward", s, g + 1, 1))
    return steps


def store_kernel(*refs):
    count = len(refs) // 2
    sem = refs[-1]
    copies = []
    for i in range(count):
        step = refs[i].shape[0] // STORE_PIECES
        for k in range(STORE_PIECES):
            rows = pl.ds(k * step, step)
            copies.append(pltpu.make_async_copy(refs[i].at[rows], refs[count + i].at[rows], sem.at[i, k]))
    for copy in copies:
        copy.start()
    for copy in copies:
        copy.wait()


def write_out(*arrays):
    return pl.pallas_call(
        store_kernel,
        out_shape=tuple(jax.ShapeDtypeStruct(a.shape, a.dtype) for a in arrays),
        in_specs=[pl.BlockSpec(memory_space=pltpu.VMEM)] * len(arrays),
        out_specs=[pl.BlockSpec(memory_space=pltpu.HBM)] * len(arrays),
        scratch_shapes=[pltpu.SemaphoreType.DMA((len(arrays), STORE_PIECES))],
        compiler_params=pltpu.CompilerParams(vmem_limit_bytes=STORE_BYTES),
        name="store",
    )(*arrays)


def fused(grads, weights, targets):
    rows_dev, feat_cols = grads.shape
    n_samp = lax.axis_size("samp")
    n_feat = lax.axis_size("feat")
    dirs = targets.shape[1]
    chips = n_samp // 2
    count = -(-dirs // CHUNK)
    n_direct, n_near = [len(part) for part in split_hops(chips, PART_HOPS)]
    f32, b16 = jnp.float32, jnp.bfloat16
    vmem = pl.BlockSpec(memory_space=pltpu.VMEM)
    dma = pltpu.SemaphoreType.DMA
    scores, solved, resid = pl.pallas_call(
        functools.partial(kernel, rows_dev * n_samp, feat_cols * n_feat),
        out_shape=(
            jax.ShapeDtypeStruct((dirs, rows_dev // n_feat), f32),
            jax.ShapeDtypeStruct((dirs, feat_cols), f32),
            jax.ShapeDtypeStruct((dirs, feat_cols), f32),
        ),
        in_specs=[pl.BlockSpec(memory_space=pltpu.HBM)] * 3,
        out_specs=[vmem] * 3,
        scratch_shapes=[
            pltpu.VMEM((rows_dev, feat_cols), b16),
            pltpu.VMEM((1, rows_dev), f32),
            pltpu.VMEM((dirs, feat_cols), f32),
            pltpu.VMEM((ITERS, dirs, rows_dev), b16),
            pltpu.VMEM((ITERS, dirs, rows_dev), b16),
            pltpu.VMEM((dirs, rows_dev), f32),
            pltpu.VMEM((dirs, rows_dev), f32),
            pltpu.VMEM((dirs, LANES), f32),
            pltpu.VMEM((dirs, LANES), f32),
            pltpu.VMEM((count, 8, LANES), f32),
            pltpu.VMEM((count, 8, LANES), f32),
            pltpu.VMEM((ITERS, 2, n_near, dirs, LANES), b16),
            pltpu.VMEM((ITERS, n_near, dirs, LANES), b16),
            pltpu.VMEM((n_near, dirs, LANES), f32),
            pltpu.VMEM((ITERS, max(1, n_near - 1), dirs, LANES), b16),
            pltpu.VMEM((ITERS, max(1, n_direct), 2, dirs, LANES), b16),
            pltpu.VMEM((ITERS, 2 * n_direct + n_near - 1, dirs, LANES), b16),
            pltpu.VMEM((ITERS, chips, 2, dirs, LANES), b16),
            pltpu.VMEM((count, 8, LANES), f32),
            pltpu.VMEM((count, n_samp, LANES), f32),
            dma((2 + PIECES,)),
            dma((ITERS, count, 2)), dma((ITERS, count, 2)),
            dma((ITERS, count)), dma((ITERS, count)),
            dma((ITERS, count)), dma((ITERS, count)),
            dma((ITERS, count)), dma((ITERS, count, chips)),
            dma((ITERS, count)), dma((ITERS, count, chips)),
            dma((count,)), dma((count,)),
        ],
        compiler_params=pltpu.CompilerParams(
            collective_id=0, has_side_effects=True, vmem_limit_bytes=VMEM_BYTES),
        name="cg",
    )(grads, pltpu.with_memory_space_constraint(weights[None, :], pltpu.HBM), targets.T)
    scores, solved, resid = write_out(scores, solved, resid)
    return scores.T, solved.T, resid.T


def per_device(grads, weights, targets):
    rows_dev, feat_cols = grads.shape
    n_samp = lax.axis_size("samp")
    n_feat = lax.axis_size("feat")
    total = rows_dev * n_samp
    full_width = feat_cols * n_feat
    share = rows_dev // n_feat
    offset = lax.axis_index("feat") * share
    scaled = weights / total
    regrouped = lax.all_to_all(grads, "feat", split_axis=0, concat_axis=1, tiled=True)
    own_weights = lax.dynamic_slice_in_dim(scaled, offset, share, 0)

    def column_norms(resid):
        squares = jnp.sum(resid * resid, axis=0)
        parts = (squares,)
        return lax.psum((parts[0],), "feat")

    solution = jnp.zeros_like(targets)
    resid = targets
    direction = targets
    accum = jnp.zeros((share, targets.shape[1]), jnp.float32)
    norm_now = column_norms(resid)[0]
    for step in range(ITERS):
        packed = direction.astype(jnp.bfloat16)
        sample_rows = jnp.dot(
            regrouped,
            lax.all_gather(packed, "feat", axis=0, tiled=True),
            preferred_element_type=jnp.float32,
        )
        weighted = (sample_rows * own_weights[:, None]).astype(jnp.bfloat16)
        partial_image = lax.psum_scatter(
            lax.dot_general(
                regrouped, weighted, (((0,), (0,)), ((), ())), preferred_element_type=jnp.float32
            ).astype(jnp.bfloat16),
            "feat",
            scatter_dimension=0,
            tiled=True,
        ).astype(jnp.float32)
        own_rows = sample_rows
        apply_own_weights = own_weights
        image = lax.psum(partial_image, "samp") + damping_term * direction
        own_rows, own_weights, image = (own_rows, apply_own_weights, image)
        curvature = lax.psum(jnp.sum(direction * image, axis=0), "feat")
        alpha = norm_now / curvature
        solution = solution + alpha * direction
        resid = resid - alpha * image
        accum = accum + alpha * own_rows
        if step + 1 < ITERS:
            sums = column_norms(resid)
            norm_next = sums[0]
            ratio = norm_next / norm_now
            direction = resid + ratio * direction
            norm_now = norm_next
    scores = accum / math.sqrt(full_width)
    return (scores, solution, resid)


def dispatch(grads, weights, targets):
    rows_dev, feat_cols = grads.shape
    n_samp, n_feat = lax.axis_size("samp"), lax.axis_size("feat")
    fits = (
        n_feat == 2
        and n_samp >= 4
        and n_samp & (n_samp - 1) == 0
        and feat_cols == n_samp * LANES
        and rows_dev % (2 * LANES) == 0
        and targets.shape[1] % CHUNK == 0
        and targets.shape[1] <= LANES
    )
    return (fused if fits else per_device)(grads, weights, targets)


def solution(mesh):
    return jax.shard_map(
        dispatch,
        mesh=mesh,
        in_specs=(P("samp", "feat"), P("samp"), P("feat", None)),
        out_specs=(P(("samp", "feat"), None), P("feat", None), P("feat", None)),
        check_vma=False,
    )
```
